512 devices in a mesh: expert: 32 (over z, y_hi, core), ctx: 16 (over x, y_lo).
Axes of the slice: x: 4, y: 8 (y_hi: 2, y_lo: 4; y = y_hi * 4 + y_lo), z: 8, core: 2. Of those that a mesh axis runs over, the one named last changes fastest.
Arguments:
- query_latent: bfloat16 [4096, 128, 512], P('ctx', 'expert'), may hold values from -3 to 3
- query_rope: bfloat16 [4096, 8192], P('ctx', 'expert'), may hold values from -128 to 128
- latent_cache: bfloat16 [576, 4096], P(None, 'ctx'), may hold values from -32 to 32
- group_order: int32 [16], replicated, may hold values from 0 to 15, each once
Outputs:
- attention_out: bfloat16 [4096, 128, 512], P('ctx', 'expert')
The draws below stay inside these ranges and needn't reach their ends.
Inputs may be any that keep to these rules, and one draw needn't show every extreme that they name: `group_order`: each block index appears once.
All inputs are finite; a program needn't handle non-finite values.
Results may differ from the reference program's by a relative error of at most 0.0045.
Values may be sent and summed in bfloat16 or wider, within the bound.
No kernel may reach another device: no remote copies, remote signals or barrier semaphores. Data moves between devices by JAX's collectives and lax.ppermute only.
A program may use at most 64 MiB of HBM per device.

```python
import jax
import jax.numpy as jnp
from jax import lax

HEADS = 128
LATENT = 512
ROPE = 64
GROUP = 256
SEQ = 4096
N_CTX = 16


def attention_draw(key):
    folded = jax.random.fold_in(key, 7001)
    key_one, key_two, key_three = jax.random.split(folded, 3)
    latent_q = 0.5 * jnp.clip(jax.random.normal(key_one, (SEQ, HEADS, LATENT), jnp.float32), -6.0, 6.0)
    rope_q = 0.5 * jnp.clip(jax.random.normal(key_two, (SEQ, HEADS * ROPE), jnp.float32), -6.0, 6.0)
    keys_all = jnp.clip(jax.random.normal(key_three, (LATENT + ROPE, SEQ), jnp.float32), -6.0, 6.0)
    return (latent_q, rope_q, keys_all)


def draw_query_latent(key, part):
    return attention_draw(key)[0].astype(jnp.bfloat16)


def draw_query_rope(key, part):
    return attention_draw(key)[1].astype(jnp.bfloat16)


def draw_latent_cache(key, part):
    return attention_draw(key)[2].astype(jnp.bfloat16)


def setup_inputs(seed: int = 0) -> dict:
    splits = jax.random.split(jax.random.key(seed), 5)
    query_latent = draw_query_latent(jax.random.fold_in(splits[4], 71), 0)
    query_rope = draw_query_rope(jax.random.fold_in(splits[4], 71), 0)
    latent_cache = draw_latent_cache(jax.random.fold_in(splits[4], 71), 0)
    group_order = jax.random.permutation(splits[3], N_CTX).astype(jnp.int32)
    return {"query_latent": query_latent, "query_rope": query_rope, "latent_cache": latent_cache, "group_order": group_order}


score_scale = 192.0 ** -0.5


def attention_reference(query_latent, query_rope, latent_cache, group_order):
    seq_total = latent_cache.shape[1]
    indices = jnp.arange(seq_total, dtype=jnp.int32)
    positions = jnp.take(group_order, indices // GROUP) * GROUP + indices % GROUP
    latent_keys = latent_cache[:LATENT].astype(jnp.float32)
    rope_keys = latent_cache[LATENT:].astype(jnp.float32)
    blocks = seq_total // GROUP
    latent_blocks = query_latent.reshape(blocks, GROUP, HEADS, LATENT)
    rope_blocks = query_rope.reshape(blocks, GROUP, HEADS, ROPE)
    position_blocks = positions.reshape(blocks, GROUP)

    def one_block(inputs):
        latent_block, rope_block, position_block = inputs
        scores = jnp.einsum("qhd,dk->qhk", latent_block.astype(jnp.float32), latent_keys, precision=lax.Precision.HIGHEST)
        scores = scores + jnp.einsum("qhr,rk->qhk", rope_block.astype(jnp.float32), rope_keys, precision=lax.Precision.HIGHEST)
        visible = (positions[None, :] <= position_block[:, None])[:, None, :]
        scores = jnp.where(visible, scores * score_scale, -1e30)
        peak = jnp.max(scores, axis=-1, keepdims=True)
        exponent = jnp.where(visible, jnp.exp(scores - peak), 0.0)
        total = jnp.sum(exponent, axis=-1)
        weights = lax.optimization_barrier(exponent.astype(jnp.bfloat16)).astype(jnp.float32)
        numer = jnp.einsum("qhk,dk->qhd", weights, latent_keys, precision=lax.Precision.HIGHEST)
        return (numer / total[..., None]).astype(jnp.bfloat16)

    outputs = lax.map(one_block, (latent_blocks, rope_blocks, position_blocks))
    return outputs.reshape(seq_total, HEADS, LATENT)


def reference(query_latent, query_rope, latent_cache, group_order):
    return attention_reference(query_latent, query_rope, latent_cache, group_order)
```

```python
import functools
import math

import jax
import jax.numpy as jnp
from jax import lax
from jax.experimental import pallas as pl
from jax.experimental.pallas import tpu as pltpu
from jax.sharding import Mesh
from jax.sharding import PartitionSpec as P

LOG_SCALE = 192.0 ** (-0.5) * math.log2(math.e)
MASKED = -1e30
FLOOR = -1e29
RING = ("yh", "co", "x", "yl")
HALF = 128
WIDTH = 512
STATE = 640
f32 = jnp.float32


def split_permute(value, shift, along):
    pairs = []
    for y in range(8):
        for core in range(2):
            for x in range(4):
                to_y, to_x = y, x
                if (core == 0) == (along == 0):
                    step = shift
                    if shift == 2 and y % 2:
                        step = -2
                    to_y = (y + step) % 8
                else:
                    to_x = (x + shift) % 4
                at = lambda u, v: (((u // 4) * 2 + core) * 4 + v) * 4 + u % 4
                pairs.append((at(y, x), at(to_y, to_x)))
    return lax.ppermute(value, RING, pairs)


def keys_of(refs):
    tiles = [ref[i] for ref in refs for i in range(ref.shape[0])]
    return jnp.concatenate(tiles, axis=1)


def scores_of(queries, keys):
    return jnp.dot(queries, keys, preferred_element_type=f32)


def mix(weights, keys):
    return lax.dot_general(
        weights, keys[:WIDTH], (((1,), (1,)), ((), ())), preferred_element_type=f32
    )


def row_bias(seen_ref, first, count):
    parts = []
    for i in range(count):
        value = jnp.where(seen_ref[first + i] > 0, 0.0, MASKED).astype(f32)
        parts.append(jnp.full((1, HALF), value, f32))
    return jnp.concatenate(parts, axis=1)


def soften(scores, peak, total):
    new_peak = jnp.maximum(peak, jnp.max(scores, axis=1, keepdims=True))
    weights = jnp.exp2(scores * LOG_SCALE - new_peak * LOG_SCALE)
    keep = jnp.exp2((peak - new_peak) * LOG_SCALE)
    total = total * keep + jnp.sum(weights, axis=1, keepdims=True)
    return weights.astype(jnp.bfloat16), new_peak, total, keep


def put_state(ref, h, numer, peak, total):
    ref[h, :, :WIDTH] = numer
    rows = numer.shape[0]
    ref[h, :, WIDTH : WIDTH + 64] = jnp.broadcast_to(peak, (rows, 64))
    ref[h, :, WIDTH + 64 :] = jnp.broadcast_to(total, (rows, 64))


def first_kernel(seen_ref, q_own, q_sib, kv_ref, own_ref, sib_ref):
    keys = keys_of([kv_ref])
    rows = q_own.shape[1]
    count = kv_ref.shape[0]
    rest = row_bias(seen_ref, 0, count)[:, HALF:]
    lane = lax.broadcasted_iota(jnp.int32, (rows, HALF), 1) + seen_ref[count] * HALF
    row = lax.broadcasted_iota(jnp.int32, (rows, HALF), 0)
    diagonal = jnp.where(lane <= row, 0.0, MASKED).astype(f32)
    work = [(q_own, own_ref, h) for h in range(4)] + [(q_sib, sib_ref, h) for h in range(4)]
    scores = scores_of(work[0][0][0], keys)
    for i, (_, out, h) in enumerate(work):
        ahead = None
        if i + 1 < len(work):
            ahead = scores_of(work[i + 1][0][work[i + 1][2]], keys)
        masked = jnp.concatenate([scores[:, :HALF] + diagonal, scores[:, HALF:] + rest], axis=1)
        floor = jnp.full((rows, 1), FLOOR, f32)
        weights, peak, total, _ = soften(masked, floor, jnp.zeros((rows, 1), f32))
        put_state(out, h, mix(weights, keys), peak, total)
        scores = ahead


def more_kernel(first, seen_ref, q_ref, state_ref, *refs):
    kvs, out = refs[:-1], refs[-1]
    keys = keys_of(kvs)
    bias = row_bias(seen_ref, first, keys.shape[1] // HALF)
    scores = scores_of(q_ref[0], keys)
    for h in range(4):
        ahead = scores_of(q_ref[h + 1], keys) if h < 3 else None
        peak = state_ref[h, :, WIDTH : WIDTH + 1]
        total = state_ref[h, :, WIDTH + 64 : WIDTH + 65]
        weights, peak, total, keep = soften(scores + bias, peak, total)
        put_state(out, h, state_ref[h, :, :WIDTH] * keep + mix(weights, keys), peak, total)
        scores = ahead


def last_kernel(first, seen_ref, q_ref, state_ref, other_ref, *refs):
    kvs, out = refs[:-1], refs[-1]
    keys = keys_of(kvs)
    bias = row_bias(seen_ref, first, keys.shape[1] // HALF)
    scores = scores_of(q_ref[0], keys)
    for h in range(4):
        ahead = scores_of(q_ref[h + 1], keys) if h < 3 else None
        peak = state_ref[h, :, WIDTH : WIDTH + 1]
        total = state_ref[h, :, WIDTH + 64 : WIDTH + 65]
        other_peak = other_ref[h, :, WIDTH : WIDTH + 1]
        other_total = other_ref[h, :, WIDTH + 64 : WIDTH + 65]
        floor = jnp.maximum(peak, other_peak)
        weights, top, extra, _ = soften(scores + bias, floor, jnp.zeros_like(total))
        mine = jnp.exp2((peak - top) * LOG_SCALE)
        theirs = jnp.exp2((other_peak - top) * LOG_SCALE)
        total = total * mine + other_total * theirs + extra
        numer = state_ref[h, :, :WIDTH] * mine + other_ref[h, :, :WIDTH] * theirs
        numer = numer + mix(weights, keys)
        out[:, h, :] = (numer * (1.0 / total)).astype(jnp.bfloat16)
        scores = ahead


VM = pl.BlockSpec(memory_space=pltpu.VMEM)
SM = pl.BlockSpec(memory_space=pltpu.SMEM)


def call(kernel, name, out_shape, heads, pieces, args, aliases=None):
    keys = pieces * HALF
    cost = pl.CostEstimate(
        flops=2 * heads * 256 * keys * (WIDTH * 2 + 64) * 2,
        bytes_accessed=4_000_000,
        transcendentals=heads * 256 * keys,
    )
    many = isinstance(out_shape, list)
    return pl.pallas_call(
        kernel,
        out_shape=out_shape,
        in_specs=[SM] + [VM] * (len(args) - 1),
        out_specs=[VM] * len(out_shape) if many else VM,
        input_output_aliases=aliases or {},
        compiler_params=pltpu.CompilerParams(vmem_limit_bytes=24 * 2**20),
        cost_estimate=cost,
        name=name,
    )(*args)


def body(query_latent, query_rope, latent_cache, group_order):
    rows, heads, _ = query_latent.shape
    core = lax.axis_index("co")
    x, y = lax.axis_index("x"), lax.axis_index("yl")
    half = jnp.where(core == 0, latent_cache[:, :HALF], latent_cache[:, HALF:])
    near = [split_permute(half, shift, 0) for shift in (1, -1, 2)]
    rope = query_rope.reshape(rows, heads, -1)
    queries = jnp.concatenate([query_latent, rope], axis=2).transpose(1, 0, 2)
    twin = lax.ppermute(queries, "co", [(0, 1), (1, 0)])
    bundle = jnp.stack([half] + near)
    far = [split_permute(bundle, shift, 1) for shift in (1, -1, 2)]

    step = jnp.array([0, -1, 1, 2], jnp.int32)
    inner, outer = jnp.tile(step, 4), jnp.repeat(step, 4)
    along_y = jnp.where(core == 0, inner, outer)
    along_x = jnp.where(core == 0, outer, inner)
    block = ((x + along_x) % 4) * 4 + (y + along_y) % 4
    orders = jnp.sum(
        jnp.where(block[:, None] == jnp.arange(16)[None, :], group_order[None, :], 0), axis=1
    )
    seen = (orders <= orders[0]).astype(jnp.int32)
    seen = jnp.concatenate([seen[:4], core[None].astype(jnp.int32), seen[4:]])

    state = jax.ShapeDtypeStruct((heads, rows, STATE), f32)
    own, sib = call(
        first_kernel, "attend_near", [state, state], 8, 4, [seen, queries, twin, bundle]
    )
    two = functools.partial(more_kernel, 5)
    one = functools.partial(more_kernel, 13)
    sib = call(two, "attend_mid_sib", state, 4, 8, [seen, twin, sib, far[0], far[1]], {2: 0})
    sib = call(one, "attend_far_sib", state, 4, 4, [seen, twin, sib, far[2]], {2: 0})
    other = lax.ppermute(sib, "co", [(0, 1), (1, 0)])
    own = call(two, "attend_mid_own", state, 4, 8, [seen, queries, own, far[0], far[1]], {2: 0})
    out = jax.ShapeDtypeStruct((rows, heads, WIDTH), jnp.bfloat16)
    last = functools.partial(last_kernel, 13)
    return call(last, "attend_far_own", out, 4, 4, [seen, queries, own, other, far[2]])


def solution(mesh):
    depth = mesh.shape["expert"] // 4
    torus = Mesh(mesh.devices.reshape(depth, 2, 2, 4, 4), ("z",) + RING)
    expert, ctx = ("z", "yh", "co"), ("x", "yl")
    placed = (P(ctx, expert, None), P(ctx, expert), P(None, ctx), P())
    return jax.shard_map(
        body, mesh=torus, in_specs=placed, out_specs=P(ctx, expert, None), check_vma=False
    )
```

```python
import functools
import math

import jax
import jax.numpy as jnp
from jax import lax
from jax.experimental import pallas as pl
from jax.experimental.pallas import tpu as pltpu
from jax.sharding import Mesh
from jax.sharding import PartitionSpec as P


LOG_SCALE = 192.0 ** (-0.5) * math.log2(math.e)
MASKED = -1e30
FLOOR = -1e29
RING = ("yh", "co", "x", "yl")
HALF = 128
VMEM_MIB = 16
QUERY = 640
USED = 576
OUTER = (-1, 1, 2)
WIDTH = 512
STATE = 768
PEAK = slice(512, 640)
TOTAL = slice(640, 768)
f32 = jnp.float32


def split_permute(value, shift, along):
    pairs = []
    for y in range(8):
        for core in range(2):
            for x in range(4):
                to_y, to_x = y, x
                if (core == 0) == (along == 0):
                    step = shift
                    if shift == 2 and y % 2:
                        step = -2
                    to_y = (y + step) % 8
                else:
                    to_x = (x + shift) % 4
                at = lambda u, v: (((u // 4) * 2 + core) * 4 + v) * 4 + u % 4
                pairs.append((at(y, x), at(to_y, to_x)))
    return lax.ppermute(value, RING, pairs)


def near_groups():
    groups = []
    for half in range(2):
        at = lambda core, x, y: ((half * 2 + core) * 4 + x) * 4 + y
        groups += [[at(0, x, y) for y in range(4)] for x in range(4)]
        groups += [[at(1, x, y) for x in range(4)] for y in range(4)]
    return groups


def keys_of(refs):
    tiles = [ref[i] for ref in refs for i in range(ref.shape[0])]
    return jnp.concatenate(tiles, axis=1)


def scores_of(queries, keys):
    return jnp.dot(queries[:, :USED], keys, preferred_element_type=f32)


def mix(weights, keys):
    return lax.dot_general(
        weights, keys[:WIDTH], (((1,), (1,)), ((), ())), preferred_element_type=f32
    )


def soften(parts, peak, total):
    top = parts[0]
    for part in parts[1:]:
        top = jnp.maximum(top, part)
    row_top = jnp.max(top, axis=1, keepdims=True)
    new_peak = jnp.maximum(peak, jnp.broadcast_to(row_top, top.shape))
    offset = new_peak * LOG_SCALE
    weights = [jnp.exp2(part * LOG_SCALE - offset) for part in parts]
    keep = jnp.exp2(peak * LOG_SCALE - offset)
    added = weights[0]
    for part in weights[1:]:
        added = added + part
    total = added if total is None else total * keep + added
    return jnp.concatenate([w.astype(jnp.bfloat16) for w in weights], axis=1), new_peak, total, keep


def pieces_of(scores):
    return [scores[:, i : i + HALF] for i in range(0, scores.shape[1], HALF)]


def block_of(place, inner, outer):
    core, x, y = place
    at_y = jnp.where(core == 0, inner, (y + outer + 4) % 4)
    at_x = jnp.where(core == 0, (x + outer + 4) % 4, inner)
    return at_x * 4 + at_y


def here(place_ref):
    return place_ref[0], place_ref[1], place_ref[2]


def masked_pieces(scores, order_ref, place_ref, parts):
    place = here(place_ref)
    mine = order_ref[place[1] * 4 + place[2]]
    pieces = pieces_of(scores)
    for i, part in enumerate(pieces):
        block = block_of(place, i % 4, OUTER[parts[i // 4]])
        pieces[i] = jnp.where(order_ref[block] < mine, part, MASKED)
    return pieces


def scaled(numer, factor):
    return jnp.concatenate([part * factor for part in pieces_of(numer)], axis=1)


def put_state(ref, h, numer, peak, total):
    ref[h, :, :WIDTH] = numer
    ref[h, :, PEAK] = peak
    ref[h, :, TOTAL] = total


def near_kernel(order_ref, place_ref, q_ref, kv_ref, out, *keep):
    for ref in keep:
        ref[...] = q_ref[...]
    keys = keys_of([kv_ref])
    rows = q_ref.shape[1]
    lane = lax.broadcasted_iota(jnp.int32, (rows, HALF), 1)
    place = here(place_ref)
    mine = order_ref[place[1] * 4 + place[2]]
    limits = []
    for i in range(4):
        order = order_ref[block_of(place, i, 0)]
        limit = jnp.where(order < mine, 4096, -4096)
        limits.append(jnp.where(order == mine, -HALF * place[0], limit))
    ahead_by = lane - lax.broadcasted_iota(jnp.int32, (rows, HALF), 0)
    scores = scores_of(q_ref[0], keys)
    for h in range(4):
        ahead = scores_of(q_ref[h + 1], keys) if h < 3 else None
        parts = [
            jnp.where(ahead_by <= limit, part, MASKED)
            for limit, part in zip(limits, pieces_of(scores))
        ]
        floor = jnp.full((rows, HALF), FLOOR, f32)
        weights, peak, total, _ = soften(parts, floor, None)
        put_state(out, h, mix(weights, keys), peak, total)
        scores = ahead


def more_kernel(parts_in, order_ref, place_ref, q_ref, state_ref, *refs):
    keys = keys_of(refs[:-1])
    out = refs[-1]
    scores = scores_of(q_ref[0], keys)
    for h in range(4):
        ahead = scores_of(q_ref[h + 1], keys) if h < 3 else None
        parts = masked_pieces(scores, order_ref, place_ref, parts_in)
        weights, peak, total, keep = soften(parts, state_ref[h, :, PEAK], state_ref[h, :, TOTAL])
        numer = scaled(state_ref[h, :, :WIDTH], keep) + mix(weights, keys)
        put_state(out, h, numer, peak, total)
        scores = ahead


def last_kernel(parts_in, order_ref, place_ref, q_ref, state_ref, other_ref, kv_ref, out):
    keys = keys_of([kv_ref])
    scores = scores_of(q_ref[0], keys)
    for h in range(4):
        ahead = scores_of(q_ref[h + 1], keys) if h < 3 else None
        parts = masked_pieces(scores, order_ref, place_ref, parts_in)
        peak, other_peak = state_ref[h, :, PEAK], other_ref[h, :, PEAK]
        floor = jnp.maximum(peak, other_peak)
        weights, top, added, _ = soften(parts, floor, None)
        mine = jnp.exp2((peak - top) * LOG_SCALE)
        theirs = jnp.exp2((other_peak - top) * LOG_SCALE)
        total = state_ref[h, :, TOTAL] * mine + other_ref[h, :, TOTAL] * theirs + added
        share = 1.0 / jnp.sum(total, axis=1, keepdims=True)
        numer = scaled(state_ref[h, :, :WIDTH], mine) + scaled(other_ref[h, :, :WIDTH], theirs)
        numer = numer + mix(weights, keys)
        out[:, h, :] = (numer * share).astype(jnp.bfloat16)
        scores = ahead


def prepare_kernel(latent_ref, rope_ref, out):
    for h in range(4):
        out[h, :, :WIDTH] = latent_ref[:, h, :]
        rope = rope_ref[:, h * 64 : h * 64 + 64]
        out[h, :, WIDTH:] = jnp.concatenate([rope, jnp.zeros_like(rope)], axis=1)


def prepare(latent, rope):
    rows, heads, _ = latent.shape
    return pl.pallas_call(
        prepare_kernel,
        grid=(4,),
        out_shape=jax.ShapeDtypeStruct((heads, rows, QUERY), jnp.bfloat16),
        in_specs=[
            pl.BlockSpec((rows // 4, heads, WIDTH), lambda i: (i, 0, 0)),
            pl.BlockSpec((rows // 4, heads * 64), lambda i: (i, 0)),
        ],
        out_specs=pl.BlockSpec((heads, rows // 4, QUERY), lambda i: (0, i, 0)),
        compiler_params=pltpu.CompilerParams(vmem_limit_bytes=VMEM_MIB * 2**20),
        cost_estimate=pl.CostEstimate(flops=1 << 30, bytes_accessed=2_000_000, transcendentals=0),
        name="prepare",
    )(latent, rope)


def spread_kernel(place_ref, cache_ref, out):
    for i in range(4):
        out[i] = cache_ref[...]


def spread(cache, place):
    rows = cache.shape[0]
    copies = pl.pallas_call(
        spread_kernel,
        grid_spec=pltpu.PrefetchScalarGridSpec(
            num_scalar_prefetch=1,
            grid=(1,),
            in_specs=[pl.BlockSpec((rows, HALF), lambda i, place: (0, place[0]))],
            out_specs=pl.BlockSpec((4, rows, HALF), lambda i, place: (0, 0, 0)),
        ),
        out_shape=jax.ShapeDtypeStruct((4, rows, HALF), cache.dtype),
        compiler_params=pltpu.CompilerParams(vmem_limit_bytes=VMEM_MIB * 2**20),
        name="spread",
    )(place, cache)
    return copies.reshape(4 * rows, HALF)


VM = pl.BlockSpec(memory_space=pltpu.VMEM)
SM = pl.BlockSpec(memory_space=pltpu.SMEM)


def call(kernel, out_shape, pieces, where, args, aliases=None):
    heads, keys = 4, pieces * HALF
    cost = pl.CostEstimate(
        flops=2 * heads * 256 * keys * (WIDTH * 2 + 64) * 2,
        bytes_accessed=4_000_000,
        transcendentals=heads * 256 * keys,
    )
    args = [*where, *args]
    specs = [SM] * len(where) + [VM] * (len(args) - len(where))
    return pl.pallas_call(
        kernel,
        out_shape=out_shape,
        in_specs=specs,
        out_specs=[VM] * len(out_shape) if isinstance(out_shape, list) else VM,
        input_output_aliases=aliases or {},
        compiler_params=pltpu.CompilerParams(vmem_limit_bytes=VMEM_MIB * 2**20),
        cost_estimate=cost,
    )(*args)


def attend(query_latent, query_rope, latent_cache, group_order):
    rows, heads, _ = query_latent.shape
    core = lax.axis_index("co")
    x, y = lax.axis_index("x"), lax.axis_index("yl")
    where = [group_order, jnp.stack([core, x, y]).astype(jnp.int32)]
    copies = spread(latent_cache, where[1])
    bundle = lax.all_to_all(copies, RING, 0, 0, axis_index_groups=near_groups(), tiled=True)
    queries = prepare(query_latent, query_rope)
    bundle = bundle.reshape(4, WIDTH + 64, HALF)
    far = []
    for shift in (1, -1, 2):
        far.append(split_permute(bundle, shift, 1))
    twin = lax.ppermute(queries, "co", [(0, 1), (1, 0)])

    state = jax.ShapeDtypeStruct((heads, rows, STATE), f32)

    def more(queries, state_in, *parts):
        kernel = functools.partial(more_kernel, parts)
        args = [queries, state_in, *(far[part] for part in parts)]
        return call(kernel, state, 4 * len(parts), where, args, {3: 0})

    own = call(near_kernel, state, 4, where, [queries, bundle])
    packed = jax.ShapeDtypeStruct(twin.shape, twin.dtype)
    sib, twin = call(near_kernel, [state, packed], 4, where, [twin, bundle])
    sib = more(twin, sib, 0)
    sib = more(twin, sib, 1, 2)
    other = lax.ppermute(sib, "co", [(0, 1), (1, 0)])
    own = more(queries, own, 0, 1)
    out = jax.ShapeDtypeStruct((rows, heads, WIDTH), jnp.bfloat16)
    last = functools.partial(last_kernel, (2,))
    return call(last, out, 4, where, [queries, own, other, far[2]])


def solution(mesh):
    depth = mesh.shape["expert"] // 4
    torus = Mesh(mesh.devices.reshape(depth, 2, 2, 4, 4), ("z",) + RING)
    expert, ctx = ("z", "yh", "co"), ("x", "yl")
    placed = (P(ctx, expert, None), P(ctx, expert), P(None, ctx), P())
    return jax.shard_map(
        attend, mesh=torus, in_specs=placed, out_specs=P(ctx, expert, None), check_vma=False
    )
```

```python
import functools
import math

import jax
import jax.numpy as jnp
from jax import lax
from jax.experimental import pallas as pl
from jax.experimental.pallas import tpu as pltpu
from jax.sharding import Mesh
from jax.sharding import PartitionSpec as P


LOG_SCALE = 192.0 ** (-0.5) * math.log2(math.e)
MASKED = -1e30
FLOOR = -1e29
RING = ("yh", "co", "x", "yl")
HALF = 128
VMEM_MIB = 16
QUERY = 640
USED = 576
OUTER = (-1, 1, 2)
WIDTH = 512
STATE = 768
PEAK = slice(512, 640)
TOTAL = slice(640, 768)
f32 = jnp.float32
VM = pl.BlockSpec(memory_space=pltpu.VMEM)
SM = pl.BlockSpec(memory_space=pltpu.SMEM)


def split_permute(value, shift, along):
    pairs = []
    for y in range(8):
        for core in range(2):
            for x in range(4):
                to_y, to_x = y, x
                if (core == 0) == (along == 0):
                    step = shift
                    if shift == 2 and y % 2:
                        step = -2
                    to_y = (y + step) % 8
                else:
                    to_x = (x + shift) % 4
                at = lambda u, v: (((u // 4) * 2 + core) * 4 + v) * 4 + u % 4
                pairs.append((at(y, x), at(to_y, to_x)))
    return lax.ppermute(value, RING, pairs)


def near_groups():
    groups = []
    for half in range(2):
        at = lambda core, x, y: ((half * 2 + core) * 4 + x) * 4 + y
        groups += [[at(0, x, y) for y in range(4)] for x in range(4)]
        groups += [[at(1, x, y) for x in range(4)] for y in range(4)]
    return groups


def keys_of(refs):
    tiles = [ref[i] for ref in refs for i in range(ref.shape[0])]
    return jnp.concatenate(tiles, axis=1)


def scores_of(queries, keys):
    return jnp.dot(queries[:, :USED], keys, preferred_element_type=f32)


def mix(weights, keys):
    return lax.dot_general(
        weights, keys[:WIDTH], (((1,), (1,)), ((), ())), preferred_element_type=f32
    )


def soften(parts, peak, total):
    top = parts[0]
    for part in parts[1:]:
        top = jnp.maximum(top, part)
    row_top = jnp.max(top, axis=1, keepdims=True)
    new_peak = jnp.maximum(peak, jnp.broadcast_to(row_top, top.shape))
    offset = new_peak * LOG_SCALE
    weights = [jnp.exp2(part * LOG_SCALE - offset) for part in parts]
    keep = jnp.exp2(peak * LOG_SCALE - offset)
    added = weights[0]
    for part in weights[1:]:
        added = added + part
    total = added if total is None else total * keep + added
    return jnp.concatenate([w.astype(jnp.bfloat16) for w in weights], axis=1), new_peak, total, keep


def pieces_of(scores):
    return [scores[:, i : i + HALF] for i in range(0, scores.shape[1], HALF)]


def block_of(place, inner, outer):
    core, x, y = place
    at_y = jnp.where(core == 0, inner, (y + outer + 4) % 4)
    at_x = jnp.where(core == 0, (x + outer + 4) % 4, inner)
    return at_x * 4 + at_y


def fill_seen(order_ref, place_ref, seen_ref):
    place = place_ref[0], place_ref[1], place_ref[2]
    mine = order_ref[place[1] * 4 + place[2]]
    for i in range(16):
        order = order_ref[block_of(place, i % 4, (0, *OUTER)[i // 4])]
        limit = jnp.where(order < mine, 4096, -4096)
        limit = jnp.where(order == mine, -HALF * place[0], limit)
        seen_ref[i : i + 1, :] = jnp.full((1, HALF), limit, jnp.int32)


def masked_pieces(scores, seen_ref, parts):
    pieces = pieces_of(scores)
    for i, part in enumerate(pieces):
        row = 4 + 4 * parts[i // 4] + i % 4
        pieces[i] = jnp.where(seen_ref[row : row + 1, :] > 0, part, MASKED)
    return pieces


def scaled(numer, factor):
    return jnp.concatenate([part * factor for part in pieces_of(numer)], axis=1)


def put_state(ref, h, numer, peak, total):
    ref[h, :, :WIDTH] = numer
    ref[h, :, PEAK] = peak
    ref[h, :, TOTAL] = total


def near_kernel(seen_ref, q_ref, kv_ref, out, *keep):
    for ref in keep:
        ref[...] = q_ref[...]
    keys = keys_of([kv_ref])
    rows = q_ref.shape[1]
    lane = lax.broadcasted_iota(jnp.int32, (rows, HALF), 1)
    ahead_by = lane - lax.broadcasted_iota(jnp.int32, (rows, HALF), 0)
    scores = scores_of(q_ref[0], keys)
    for h in range(4):
        ahead = scores_of(q_ref[h + 1], keys) if h < 3 else None
        parts = [
            jnp.where(ahead_by <= seen_ref[i : i + 1, :], part, MASKED)
            for i, part in enumerate(pieces_of(scores))
        ]
        floor = jnp.full((rows, HALF), FLOOR, f32)
        weights, peak, total, _ = soften(parts, floor, None)
        put_state(out, h, mix(weights, keys), peak, total)
        scores = ahead


def more_kernel(parts_in, seen_ref, q_ref, state_ref, *refs):
    keys = keys_of(refs[:-1])
    out = refs[-1]
    scores = scores_of(q_ref[0], keys)
    for h in range(4):
        ahead = scores_of(q_ref[h + 1], keys) if h < 3 else None
        parts = masked_pieces(scores, seen_ref, parts_in)
        weights, peak, total, keep = soften(parts, state_ref[h, :, PEAK], state_ref[h, :, TOTAL])
        numer = scaled(state_ref[h, :, :WIDTH], keep) + mix(weights, keys)
        put_state(out, h, numer, peak, total)
        scores = ahead


def send_kernel(parts_in, seen_ref, q_ref, state_ref, *refs):
    keys = keys_of(refs[:-1])
    out = refs[-1]
    scores = scores_of(q_ref[0], keys)
    rows = q_ref.shape[1]
    lane = lax.broadcasted_iota(jnp.int32, (rows, HALF), 1)
    for h in range(4):
        ahead = scores_of(q_ref[h + 1], keys) if h < 3 else None
        parts = masked_pieces(scores, seen_ref, parts_in)
        weights, peak, total, keep = soften(parts, state_ref[h, :, PEAK], state_ref[h, :, TOTAL])
        total = jnp.broadcast_to(jnp.sum(total, axis=1, keepdims=True), (rows, HALF))
        some = total > 0.0
        share = jnp.where(some, 1.0 / jnp.where(some, total, 1.0), 0.0)
        size = jnp.log2(jnp.where(some, total, 1.0)) + peak * LOG_SCALE
        size = jnp.where(some, size, FLOOR)
        high = size.astype(jnp.bfloat16).astype(f32)
        middle = (size - high).astype(jnp.bfloat16).astype(f32)
        low = size - high - middle
        tag = jnp.where(lane == 0, high, jnp.where(lane == 1, middle, low))
        out[h, :, WIDTH:] = jnp.where(lane < 3, tag, 0.0).astype(jnp.bfloat16)
        numer = scaled(state_ref[h, :, :WIDTH], keep * share)
        for i, part in enumerate(pieces_of(mix(weights, keys))):
            span = slice(i * HALF, (i + 1) * HALF)
            out[h, :, span] = (numer[:, span] + part * share).astype(jnp.bfloat16)
        scores = ahead


def last_kernel(parts_in, seen_ref, q_ref, state_ref, other_ref, kv_ref, out, held):
    keys = keys_of([kv_ref])
    scores = scores_of(q_ref[0], keys)
    for h in range(4):
        ahead = scores_of(q_ref[h + 1], keys) if h < 3 else None
        parts = masked_pieces(scores, seen_ref, parts_in)
        peak = state_ref[h, :, PEAK]
        size = jnp.sum(other_ref[h, :, WIDTH:].astype(f32), axis=1, keepdims=True)
        size = jnp.broadcast_to(size, peak.shape)
        floor = jnp.maximum(peak, size * (1.0 / LOG_SCALE))
        weights, top, added, _ = soften(parts, floor, None)
        mine = jnp.exp2((peak - top) * LOG_SCALE)
        theirs = jnp.exp2(size - top * LOG_SCALE)
        total = jnp.sum(state_ref[h, :, TOTAL] * mine + added, axis=1, keepdims=True)
        share = 1.0 / (jnp.broadcast_to(total, peak.shape) + theirs)
        numer = scaled(state_ref[h, :, :WIDTH], mine * share)
        numer = numer + scaled(other_ref[h, :, :WIDTH].astype(f32), theirs * share)
        held[h] = (numer + scaled(mix(weights, keys), share)).astype(jnp.bfloat16)
        scores = ahead
    out[...] = jnp.swapaxes(held[...], 0, 1)


def prepare_kernel(order_ref, place_ref, latent_ref, rope_ref, out, seen_ref):
    for h in range(4):
        out[h, :, :WIDTH] = latent_ref[:, h, :]
        rope = rope_ref[:, h * 64 : h * 64 + 64]
        out[h, :, WIDTH:] = jnp.concatenate([rope, jnp.zeros_like(rope)], axis=1)

    @pl.when(pl.program_id(0) == 0)
    def _():
        fill_seen(order_ref, place_ref, seen_ref)


def prepare(order, place, latent, rope):
    rows, heads, _ = latent.shape
    return pl.pallas_call(
        prepare_kernel,
        grid=(4,),
        out_shape=[
            jax.ShapeDtypeStruct((heads, rows, QUERY), jnp.bfloat16),
            jax.ShapeDtypeStruct((16, HALF), jnp.int32),
        ],
        in_specs=[
            SM,
            SM,
            pl.BlockSpec((rows // 4, heads, WIDTH), lambda i: (i, 0, 0)),
            pl.BlockSpec((rows // 4, heads * 64), lambda i: (i, 0)),
        ],
        out_specs=[
            pl.BlockSpec((heads, rows // 4, QUERY), lambda i: (0, i, 0)),
            pl.BlockSpec((16, HALF), lambda i: (0, 0)),
        ],
        compiler_params=pltpu.CompilerParams(vmem_limit_bytes=VMEM_MIB * 2**20),
        cost_estimate=pl.CostEstimate(flops=1 << 30, bytes_accessed=2_000_000, transcendentals=0),
        name="prepare",
    )(order, place, latent, rope)


def spread_kernel(place_ref, cache_ref, out):
    for i in range(4):
        out[i] = cache_ref[...]


def spread(cache, place):
    rows = cache.shape[0]
    copies = pl.pallas_call(
        spread_kernel,
        grid_spec=pltpu.PrefetchScalarGridSpec(
            num_scalar_prefetch=1,
            grid=(1,),
            in_specs=[pl.BlockSpec((rows, HALF), lambda i, place: (0, place[0]))],
            out_specs=pl.BlockSpec((4, rows, HALF), lambda i, place: (0, 0, 0)),
        ),
        out_shape=jax.ShapeDtypeStruct((4, rows, HALF), cache.dtype),
        compiler_params=pltpu.CompilerParams(vmem_limit_bytes=VMEM_MIB * 2**20),
        name="spread",
    )(place, cache)
    return copies.reshape(4 * rows, HALF)


def call(kernel, out_shape, pieces, args, aliases=None, scratch=()):
    heads, keys = 4, pieces * HALF
    cost = pl.CostEstimate(
        flops=2 * heads * 256 * keys * (WIDTH * 2 + 64) * 2,
        bytes_accessed=4_000_000,
        transcendentals=heads * 256 * keys,
    )
    return pl.pallas_call(
        kernel,
        out_shape=out_shape,
        in_specs=[VM] * len(args),
        out_specs=[VM] * len(out_shape) if isinstance(out_shape, list) else VM,
        input_output_aliases=aliases or {},
        scratch_shapes=scratch,
        compiler_params=pltpu.CompilerParams(vmem_limit_bytes=VMEM_MIB * 2**20),
        cost_estimate=cost,
    )(*args)


def attend(query_latent, query_rope, latent_cache, group_order):
    rows, heads, _ = query_latent.shape
    core = lax.axis_index("co")
    x, y = lax.axis_index("x"), lax.axis_index("yl")
    where = [group_order, jnp.stack([core, x, y]).astype(jnp.int32)]
    copies = spread(pltpu.with_memory_space_constraint(latent_cache, pltpu.HBM), where[1])
    bundle = lax.all_to_all(copies, RING, 0, 0, axis_index_groups=near_groups(), tiled=True)
    queries, seen = prepare(*where, query_latent, query_rope)
    bundle = bundle.reshape(4, WIDTH + 64, HALF)
    far = []
    for shift in (1, -1, 2):
        far.append(split_permute(bundle, shift, 1))
    twin = lax.ppermute(queries, "co", [(0, 1), (1, 0)])

    state = jax.ShapeDtypeStruct((heads, rows, STATE), f32)

    def more(queries, state_in, *parts):
        kernel = functools.partial(more_kernel, parts)
        args = [seen, queries, state_in, *(far[part] for part in parts)]
        return call(kernel, state, 4 * len(parts), args, {2: 0})

    packed = jax.ShapeDtypeStruct(twin.shape, twin.dtype)
    own = call(near_kernel, state, 4, [seen, queries, bundle])
    sib, twin = call(near_kernel, [state, packed], 4, [seen, twin, bundle])
    sib = more(twin, sib, 0)
    own = more(queries, own, 0)
    send = functools.partial(send_kernel, (1, 2))
    sib = call(send, packed, 8, [seen, twin, sib, far[1], far[2]])
    other = lax.ppermute(sib, "co", [(0, 1), (1, 0)])
    own = more(queries, own, 1)
    out = jax.ShapeDtypeStruct((rows, heads, WIDTH), jnp.bfloat16)
    last = functools.partial(last_kernel, (2,))
    held = pltpu.VMEM((heads, rows, WIDTH), jnp.bfloat16)
    return call(last, out, 4, [seen, queries, own, other, far[2]], scratch=[held])


def solution(mesh):
    depth = mesh.shape["expert"] // 4
    torus = Mesh(mesh.devices.reshape(depth, 2, 2, 4, 4), ("z",) + RING)
    expert, ctx = ("z", "yh", "co"), ("x", "yl")
    placed = (P(ctx, expert, None), P(ctx, expert), P(None, ctx), P())
    return jax.shard_map(
        attend, mesh=torus, in_specs=placed, out_specs=P(ctx, expert, None), check_vma=False
    )
```

```python
import functools
import math

import jax
import jax.numpy as jnp
from jax import lax
from jax.experimental import pallas as pl
from jax.experimental.pallas import tpu as pltpu
from jax.sharding import Mesh
from jax.sharding import PartitionSpec as P


LOG_SCALE = 192.0 ** (-0.5) * math.log2(math.e)
MASKED = -1e30
FLOOR = -1e29
RING = ("yh", "co", "x", "yl")
HALF = 128
VMEM_MIB = 16
QUERY = 640
USED = 576
OUTER = (-1, 1, 2)
WIDTH = 512
STATE = 768
PEAK = slice(512, 640)
TOTAL = slice(640, 768)
f32 = jnp.float32
VM = pl.BlockSpec(memory_space=pltpu.VMEM)
SM = pl.BlockSpec(memory_space=pltpu.SMEM)


def split_permute(value, shift, along):
    pairs = []
    for y in range(8):
        for core in range(2):
            for x in range(4):
                to_y, to_x = y, x
                if (core == 0) == (along == 0):
                    step = shift
                    if shift == 2 and y % 2:
                        step = -2
                    to_y = (y + step) % 8
                else:
                    to_x = (x + shift) % 4
                at = lambda u, v: (((u // 4) * 2 + core) * 4 + v) * 4 + u % 4
                pairs.append((at(y, x), at(to_y, to_x)))
    return lax.ppermute(value, RING, pairs)


def near_groups():
    groups = []
    for half in range(2):
        at = lambda core, x, y: ((half * 2 + core) * 4 + x) * 4 + y
        groups += [[at(0, x, y) for y in range(4)] for x in range(4)]
        groups += [[at(1, x, y) for x in range(4)] for y in range(4)]
    return groups


def keys_of(refs):
    tiles = [ref[i] for ref in refs for i in range(ref.shape[0])]
    return jnp.concatenate(tiles, axis=1)


def scores_of(queries, keys):
    return jnp.dot(queries[:, :USED], keys, preferred_element_type=f32)


def mix(weights, keys):
    return lax.dot_general(
        weights, keys[:WIDTH], (((1,), (1,)), ((), ())), preferred_element_type=f32
    )


def soften(parts, peak, total):
    top = parts[0]
    for part in parts[1:]:
        top = jnp.maximum(top, part)
    row_top = jnp.max(top, axis=1, keepdims=True)
    new_peak = jnp.maximum(peak, jnp.broadcast_to(row_top, top.shape))
    offset = new_peak * LOG_SCALE
    weights = [jnp.exp2(part * LOG_SCALE - offset) for part in parts]
    keep = jnp.exp2(peak * LOG_SCALE - offset)
    added = weights[0]
    for part in weights[1:]:
        added = added + part
    total = added if total is None else total * keep + added
    return jnp.concatenate([w.astype(jnp.bfloat16) for w in weights], axis=1), new_peak, total, keep


def pieces_of(scores):
    return [scores[:, i : i + HALF] for i in range(0, scores.shape[1], HALF)]


def block_of(place, inner, outer):
    core, x, y = place
    at_y = jnp.where(core == 0, inner, (y + outer + 4) % 4)
    at_x = jnp.where(core == 0, (x + outer + 4) % 4, inner)
    return at_x * 4 + at_y


def fill_seen(order_ref, place_ref, seen_ref):
    place = place_ref[0], place_ref[1], place_ref[2]
    mine = order_ref[place[1] * 4 + place[2]]
    for i in range(16):
        order = order_ref[block_of(place, i % 4, (0, *OUTER)[i // 4])]
        limit = jnp.where(order < mine, 4096, -4096)
        limit = jnp.where(order == mine, -HALF * place[0], limit)
        seen_ref[i : i + 1, :] = jnp.full((1, HALF), limit, jnp.int32)


def masked_pieces(scores, seen_ref, parts):
    pieces = pieces_of(scores)
    for i, part in enumerate(pieces):
        row = 4 + 4 * parts[i // 4] + i % 4
        pieces[i] = jnp.where(seen_ref[row : row + 1, :] > 0, part, MASKED)
    return pieces


def scaled(numer, factor):
    return jnp.concatenate([part * factor for part in pieces_of(numer)], axis=1)


def put_state(ref, h, numer, peak, total):
    ref[h, :, :WIDTH] = numer
    ref[h, :, PEAK] = peak
    ref[h, :, TOTAL] = total


def near_kernel(seen_ref, own_ref, twin_ref, kv_ref, own_out, sib_out, keep_ref):
    keys = keys_of([kv_ref])
    rows = own_ref.shape[1]
    lane = lax.broadcasted_iota(jnp.int32, (rows, HALF), 1)
    ahead_by = lane - lax.broadcasted_iota(jnp.int32, (rows, HALF), 0)
    work = [(own_ref, own_out, h) for h in range(4)] + [(twin_ref, sib_out, h) for h in range(4)]
    scores = scores_of(own_ref[0], keys)
    for i, (_, out, h) in enumerate(work):
        ahead = None
        if i + 1 < len(work):
            ahead = scores_of(work[i + 1][0][work[i + 1][2]], keys)
        parts = [
            jnp.where(ahead_by <= seen_ref[j : j + 1, :], part, MASKED)
            for j, part in enumerate(pieces_of(scores))
        ]
        floor = jnp.full((rows, HALF), FLOOR, f32)
        weights, peak, total, _ = soften(parts, floor, None)
        put_state(out, h, mix(weights, keys), peak, total)
        scores = ahead
    keep_ref[...] = twin_ref[...]


def more_kernel(parts_in, count, seen_ref, *refs):
    queries, states = refs[:count], refs[count : 2 * count]
    outs = refs[len(refs) - count :]
    keys = keys_of(refs[2 * count : len(refs) - count])
    work = [(q, s, out, h) for q, s, out in zip(queries, states, outs) for h in range(4)]
    scores = scores_of(work[0][0][0], keys)
    for i, (_, state, out, h) in enumerate(work):
        ahead = None
        if i + 1 < len(work):
            ahead = scores_of(work[i + 1][0][work[i + 1][3]], keys)
        parts = masked_pieces(scores, seen_ref, parts_in)
        weights, peak, total, keep = soften(parts, state[h, :, PEAK], state[h, :, TOTAL])
        numer = scaled(state[h, :, :WIDTH], keep) + mix(weights, keys)
        put_state(out, h, numer, peak, total)
        scores = ahead


def send_kernel(parts_in, seen_ref, q_ref, state_ref, *refs):
    keys = keys_of(refs[:-1])
    out = refs[-1]
    scores = scores_of(q_ref[0], keys)
    rows = q_ref.shape[1]
    lane = lax.broadcasted_iota(jnp.int32, (rows, HALF), 1)
    for h in range(4):
        ahead = scores_of(q_ref[h + 1], keys) if h < 3 else None
        parts = masked_pieces(scores, seen_ref, parts_in)
        weights, peak, total, keep = soften(parts, state_ref[h, :, PEAK], state_ref[h, :, TOTAL])
        total = jnp.broadcast_to(jnp.sum(total, axis=1, keepdims=True), (rows, HALF))
        some = total > 0.0
        share = jnp.where(some, 1.0 / jnp.where(some, total, 1.0), 0.0)
        size = jnp.log2(jnp.where(some, total, 1.0)) + peak * LOG_SCALE
        size = jnp.where(some, size, FLOOR)
        high = size.astype(jnp.bfloat16).astype(f32)
        middle = (size - high).astype(jnp.bfloat16).astype(f32)
        low = size - high - middle
        tag = jnp.where(lane == 0, high, jnp.where(lane == 1, middle, low))
        out[h, :, WIDTH:] = jnp.where(lane < 3, tag, 0.0).astype(jnp.bfloat16)
        numer = scaled(state_ref[h, :, :WIDTH], keep * share)
        for i, part in enumerate(pieces_of(mix(weights, keys))):
            span = slice(i * HALF, (i + 1) * HALF)
            out[h, :, span] = (numer[:, span] + part * share).astype(jnp.bfloat16)
        scores = ahead


def last_kernel(parts_in, seen_ref, q_ref, state_ref, other_ref, kv_ref, out, held, sems):
    keys = keys_of([kv_ref])
    heads, rows, _ = q_ref.shape
    step = rows // 4
    span = lambda c: slice(c * step, (c + 1) * step)
    flat = lambda value: value.reshape(heads * step, value.shape[-1])
    scores = scores_of(flat(q_ref[:, span(0), :]), keys)
    copies = []
    for c in range(4):
        ahead = scores_of(flat(q_ref[:, span(c + 1), :]), keys) if c < 3 else None
        parts = masked_pieces(scores, seen_ref, parts_in)
        peak = flat(state_ref[:, span(c), PEAK])
        size = flat(other_ref[:, span(c), WIDTH:]).astype(f32)
        size = jnp.broadcast_to(jnp.sum(size, axis=1, keepdims=True), peak.shape)
        floor = jnp.maximum(peak, size * (1.0 / LOG_SCALE))
        weights, top, added, _ = soften(parts, floor, None)
        mine = jnp.exp2((peak - top) * LOG_SCALE)
        theirs = jnp.exp2(size - top * LOG_SCALE)
        total = flat(state_ref[:, span(c), TOTAL]) * mine + added
        total = jnp.sum(total, axis=1, keepdims=True)
        share = 1.0 / (jnp.broadcast_to(total, peak.shape) + theirs)
        numer = scaled(flat(state_ref[:, span(c), :WIDTH]), mine * share)
        numer = numer + scaled(flat(other_ref[:, span(c), :WIDTH]).astype(f32), theirs * share)
        numer = (numer + scaled(mix(weights, keys), share)).astype(jnp.bfloat16)
        held[span(c)] = jnp.swapaxes(numer.reshape(heads, step, WIDTH), 0, 1)
        copies.append(pltpu.make_async_copy(held.at[span(c)], out.at[span(c)], sems.at[c]))
        copies[-1].start()
        scores = ahead
    for copy in copies:
        copy.wait()


def prepare_kernel(order_ref, place_ref, latent_ref, rope_ref, out, seen_ref):
    for h in range(4):
        out[h, :, :WIDTH] = latent_ref[:, h, :]
        rope = rope_ref[:, h * 64 : h * 64 + 64]
        out[h, :, WIDTH:] = jnp.concatenate([rope, jnp.zeros_like(rope)], axis=1)

    @pl.when(pl.program_id(0) == 0)
    def _():
        fill_seen(order_ref, place_ref, seen_ref)


def prepare(order, place, latent, rope):
    rows, heads, _ = latent.shape
    return pl.pallas_call(
        prepare_kernel,
        grid=(4,),
        out_shape=[
            jax.ShapeDtypeStruct((heads, rows, QUERY), jnp.bfloat16),
            jax.ShapeDtypeStruct((16, HALF), jnp.int32),
        ],
        in_specs=[
            SM,
            SM,
            pl.BlockSpec((rows // 4, heads, WIDTH), lambda i: (i, 0, 0)),
            pl.BlockSpec((rows // 4, heads * 64), lambda i: (i, 0)),
        ],
        out_specs=[
            pl.BlockSpec((heads, rows // 4, QUERY), lambda i: (0, i, 0)),
            pl.BlockSpec((16, HALF), lambda i: (0, 0)),
        ],
        compiler_params=pltpu.CompilerParams(vmem_limit_bytes=VMEM_MIB * 2**20),
        cost_estimate=pl.CostEstimate(flops=1 << 30, bytes_accessed=2_000_000, transcendentals=0),
        name="prepare",
    )(order, place, latent, rope)


def spread_kernel(place_ref, cache_ref, out):
    for i in range(4):
        out[i] = cache_ref[...]


def spread(cache, place):
    rows = cache.shape[0]
    copies = pl.pallas_call(
        spread_kernel,
        grid_spec=pltpu.PrefetchScalarGridSpec(
            num_scalar_prefetch=1,
            grid=(1,),
            in_specs=[pl.BlockSpec((rows, HALF), lambda i, place: (0, place[0]))],
            out_specs=pl.BlockSpec((4, rows, HALF), lambda i, place: (0, 0, 0)),
        ),
        out_shape=jax.ShapeDtypeStruct((4, rows, HALF), cache.dtype),
        compiler_params=pltpu.CompilerParams(vmem_limit_bytes=VMEM_MIB * 2**20),
        name="spread",
    )(place, cache)
    return copies.reshape(4 * rows, HALF)


def call(kernel, out_shape, pieces, args, aliases=None, scratch=(), out_spec=VM):
    heads, keys = 4, pieces * HALF
    cost = pl.CostEstimate(
        flops=2 * heads * 256 * keys * (WIDTH * 2 + 64) * 2,
        bytes_accessed=4_000_000,
        transcendentals=heads * 256 * keys,
    )
    return pl.pallas_call(
        kernel,
        out_shape=out_shape,
        in_specs=[VM] * len(args),
        out_specs=[VM] * len(out_shape) if isinstance(out_shape, list) else out_spec,
        input_output_aliases=aliases or {},
        scratch_shapes=scratch,
        compiler_params=pltpu.CompilerParams(vmem_limit_bytes=VMEM_MIB * 2**20),
        cost_estimate=cost,
    )(*args)


def attend(query_latent, query_rope, latent_cache, group_order):
    rows, heads, _ = query_latent.shape
    core = lax.axis_index("co")
    x, y = lax.axis_index("x"), lax.axis_index("yl")
    where = [group_order, jnp.stack([core, x, y]).astype(jnp.int32)]
    copies = spread(pltpu.with_memory_space_constraint(latent_cache, pltpu.HBM), where[1])
    bundle = lax.all_to_all(copies, RING, 0, 0, axis_index_groups=near_groups(), tiled=True)
    queries, seen = prepare(*where, query_latent, query_rope)
    bundle = bundle.reshape(4, WIDTH + 64, HALF)
    far = []
    for shift in (1, -1, 2):
        far.append(split_permute(bundle, shift, 1))
    twin = lax.ppermute(queries, "co", [(0, 1), (1, 0)])

    state = jax.ShapeDtypeStruct((heads, rows, STATE), f32)

    def more(queries, states, *parts):
        count = len(queries)
        kernel = functools.partial(more_kernel, parts, count)
        args = [seen, *queries, *states, *(far[part] for part in parts)]
        aliases = {1 + count + i: i for i in range(count)}
        return call(kernel, [state] * count, 4 * len(parts) * count, args, aliases)

    packed = jax.ShapeDtypeStruct(twin.shape, twin.dtype)
    args = [seen, queries, twin, bundle]
    own, sib, twin = call(near_kernel, [state, state, packed], 8, args)
    own, sib = more([queries, twin], [own, sib], 2)
    (sib,) = more([twin], [sib], 0)
    send = functools.partial(send_kernel, (1,))
    sib = call(send, packed, 4, [seen, twin, sib, far[1]])
    other = lax.ppermute(sib, "co", [(0, 1), (1, 0)])
    (own,) = more([queries], [own], 0)
    out = jax.ShapeDtypeStruct((rows, heads, WIDTH), jnp.bfloat16)
    last = functools.partial(last_kernel, (1,))
    scratch = [pltpu.VMEM((rows, heads, WIDTH), jnp.bfloat16), pltpu.SemaphoreType.DMA((4,))]
    args = [seen, queries, own, other, far[1]]
    hbm = pl.BlockSpec(memory_space=pltpu.HBM)
    return call(last, out, 4, args, scratch=scratch, out_spec=hbm)


def solution(mesh):
    depth = mesh.shape["expert"] // 4
    torus = Mesh(mesh.devices.reshape(depth, 2, 2, 4, 4), ("z",) + RING)
    expert, ctx = ("z", "yh", "co"), ("x", "yl")
    placed = (P(ctx, expert, None), P(ctx, expert), P(None, ctx), P())
    return jax.shard_map(
        attend, mesh=torus, in_specs=placed, out_specs=P(ctx, expert, None), check_vma=False
    )
```

```python
import functools
import math

import jax
import jax.numpy as jnp
from jax import lax
from jax.experimental import pallas as pl
from jax.experimental.pallas import tpu as pltpu
from jax.sharding import Mesh
from jax.sharding import PartitionSpec as P


LOG_SCALE = 192.0 ** (-0.5) * math.log2(math.e)
MASKED = -1e30
FLOOR = -1e29
RING = ("yh", "co", "x", "yl")
HALF = 128
VMEM_MIB = 16
QUERY = 640
USED = 576
OUTER = (-1, 1, 2)
WIDTH = 512
STATE = 768
PEAK = slice(512, 640)
TOTAL = slice(640, 768)
f32 = jnp.float32
VM = pl.BlockSpec(memory_space=pltpu.VMEM)
SM = pl.BlockSpec(memory_space=pltpu.SMEM)


def split_permute(value, shift, along):
    pairs = []
    for y in range(8):
        for core in range(2):
            for x in range(4):
                to_y, to_x = y, x
                if (core == 0) == (along == 0):
                    step = shift
                    if shift == 2 and y % 2:
                        step = -2
                    to_y = (y + step) % 8
                else:
                    to_x = (x + shift) % 4
                at = lambda u, v: (((u // 4) * 2 + core) * 4 + v) * 4 + u % 4
                pairs.append((at(y, x), at(to_y, to_x)))
    return lax.ppermute(value, RING, pairs)


def in_hbm(value):
    return pltpu.with_memory_space_constraint(value, pltpu.HBM)


def near_groups():
    groups = []
    for half in range(2):
        at = lambda core, x, y: ((half * 2 + core) * 4 + x) * 4 + y
        groups += [[at(0, x, y) for y in range(4)] for x in range(4)]
        groups += [[at(1, x, y) for x in range(4)] for y in range(4)]
    return groups


def keys_of(refs):
    tiles = [ref[i] for ref in refs for i in range(ref.shape[0])]
    return jnp.concatenate(tiles, axis=1)


def scores_of(queries, keys):
    return jnp.dot(queries[:, :USED], keys, preferred_element_type=f32)


def mix(weights, keys):
    return lax.dot_general(
        weights, keys[:WIDTH], (((1,), (1,)), ((), ())), preferred_element_type=f32
    )


def soften(parts, peak, total):
    top = parts[0]
    for part in parts[1:]:
        top = jnp.maximum(top, part)
    row_top = jnp.max(top, axis=1, keepdims=True)
    new_peak = jnp.maximum(peak, jnp.broadcast_to(row_top, top.shape))
    offset = new_peak * LOG_SCALE
    weights = [jnp.exp2(part * LOG_SCALE - offset) for part in parts]
    keep = jnp.exp2(peak * LOG_SCALE - offset)
    added = weights[0]
    for part in weights[1:]:
        added = added + part
    total = added if total is None else total * keep + added
    return jnp.concatenate([w.astype(jnp.bfloat16) for w in weights], axis=1), new_peak, total, keep


def pieces_of(scores):
    return [scores[:, i : i + HALF] for i in range(0, scores.shape[1], HALF)]


def block_of(place, inner, outer):
    core, x, y = place
    at_y = jnp.where(core == 0, inner, (y + outer + 4) % 4)
    at_x = jnp.where(core == 0, (x + outer + 4) % 4, inner)
    return at_x * 4 + at_y


def fill_seen(order_ref, place_ref, seen_ref):
    place = place_ref[0], place_ref[1], place_ref[2]
    mine = order_ref[place[1] * 4 + place[2]]
    for i in range(16):
        order = order_ref[block_of(place, i % 4, (0, *OUTER)[i // 4])]
        limit = jnp.where(order < mine, 4096, -4096)
        limit = jnp.where(order == mine, -HALF * place[0], limit)
        seen_ref[i : i + 1, :] = jnp.full((1, HALF), limit, jnp.int32)


def masked_pieces(scores, seen_ref, parts):
    pieces = pieces_of(scores)
    for i, part in enumerate(pieces):
        row = 4 + 4 * parts[i // 4] + i % 4
        pieces[i] = jnp.where(seen_ref[row : row + 1, :] > 0, part, MASKED)
    return pieces


def scaled(numer, factor):
    return jnp.concatenate([part * factor for part in pieces_of(numer)], axis=1)


def put_state(ref, h, numer, peak, total):
    ref[h, :, :WIDTH] = numer
    ref[h, :, PEAK] = peak
    ref[h, :, TOTAL] = total


def near_kernel(seen_ref, own_ref, twin_ref, kv_ref, own_out, sib_out, keep_ref):
    keys = keys_of([kv_ref])
    rows = own_ref.shape[1]
    lane = lax.broadcasted_iota(jnp.int32, (rows, HALF), 1)
    ahead_by = lane - lax.broadcasted_iota(jnp.int32, (rows, HALF), 0)
    work = [(own_ref, own_out, h) for h in range(4)] + [(twin_ref, sib_out, h) for h in range(4)]
    scores = scores_of(own_ref[0], keys)
    for i, (_, out, h) in enumerate(work):
        ahead = None
        if i + 1 < len(work):
            ahead = scores_of(work[i + 1][0][work[i + 1][2]], keys)
        parts = [
            jnp.where(ahead_by <= seen_ref[j : j + 1, :], part, MASKED)
            for j, part in enumerate(pieces_of(scores))
        ]
        floor = jnp.full((rows, HALF), FLOOR, f32)
        weights, peak, total, _ = soften(parts, floor, None)
        put_state(out, h, mix(weights, keys), peak, total)
        scores = ahead
    keep_ref[...] = twin_ref[...]


def more_kernel(parts_in, count, seen_ref, *refs):
    queries, states = refs[:count], refs[count : 2 * count]
    outs = refs[len(refs) - count :]
    keys = keys_of(refs[2 * count : len(refs) - count])
    work = [(q, s, out, h) for q, s, out in zip(queries, states, outs) for h in range(4)]
    scores = scores_of(work[0][0][0], keys)
    for i, (_, state, out, h) in enumerate(work):
        ahead = None
        if i + 1 < len(work):
            ahead = scores_of(work[i + 1][0][work[i + 1][3]], keys)
        parts = masked_pieces(scores, seen_ref, parts_in)
        weights, peak, total, keep = soften(parts, state[h, :, PEAK], state[h, :, TOTAL])
        numer = scaled(state[h, :, :WIDTH], keep) + mix(weights, keys)
        put_state(out, h, numer, peak, total)
        scores = ahead


def send_kernel(parts_in, seen_ref, q_ref, state_ref, *refs):
    keys = keys_of(refs[:-1])
    out = refs[-1]
    scores = scores_of(q_ref[0], keys)
    rows = q_ref.shape[1]
    lane = lax.broadcasted_iota(jnp.int32, (rows, HALF), 1)
    for h in range(4):
        ahead = scores_of(q_ref[h + 1], keys) if h < 3 else None
        parts = masked_pieces(scores, seen_ref, parts_in)
        weights, peak, total, keep = soften(parts, state_ref[h, :, PEAK], state_ref[h, :, TOTAL])
        total = jnp.broadcast_to(jnp.sum(total, axis=1, keepdims=True), (rows, HALF))
        some = total > 0.0
        share = jnp.where(some, 1.0 / jnp.where(some, total, 1.0), 0.0)
        size = jnp.log2(jnp.where(some, total, 1.0)) + peak * LOG_SCALE
        size = jnp.where(some, size, FLOOR)
        high = size.astype(jnp.bfloat16).astype(f32)
        middle = (size - high).astype(jnp.bfloat16).astype(f32)
        low = size - high - middle
        tag = jnp.where(lane == 0, high, jnp.where(lane == 1, middle, low))
        out[h, :, WIDTH:] = jnp.where(lane < 3, tag, 0.0).astype(jnp.bfloat16)
        numer = scaled(state_ref[h, :, :WIDTH], keep * share)
        for i, part in enumerate(pieces_of(mix(weights, keys))):
            span = slice(i * HALF, (i + 1) * HALF)
            out[h, :, span] = (numer[:, span] + part * share).astype(jnp.bfloat16)
        scores = ahead


def last_kernel(parts_in, seen_ref, q_ref, state_ref, other_ref, kv_ref, out, held, sems):
    keys = keys_of([kv_ref])
    heads, rows, _ = q_ref.shape
    step = rows // 4
    span = lambda c: slice(c * step, (c + 1) * step)
    flat = lambda value: value.reshape(heads * step, value.shape[-1])
    scores = scores_of(flat(q_ref[:, span(0), :]), keys)
    copies = []
    for c in range(4):
        ahead = scores_of(flat(q_ref[:, span(c + 1), :]), keys) if c < 3 else None
        parts = masked_pieces(scores, seen_ref, parts_in)
        peak = flat(state_ref[:, span(c), PEAK])
        size = flat(other_ref[:, span(c), WIDTH:]).astype(f32)
        size = jnp.broadcast_to(jnp.sum(size, axis=1, keepdims=True), peak.shape)
        floor = jnp.maximum(peak, size * (1.0 / LOG_SCALE))
        weights, top, added, _ = soften(parts, floor, None)
        mine = jnp.exp2((peak - top) * LOG_SCALE)
        theirs = jnp.exp2(size - top * LOG_SCALE)
        total = flat(state_ref[:, span(c), TOTAL]) * mine + added
        total = jnp.sum(total, axis=1, keepdims=True)
        share = 1.0 / (jnp.broadcast_to(total, peak.shape) + theirs)
        numer = scaled(flat(state_ref[:, span(c), :WIDTH]), mine * share)
        numer = numer + scaled(flat(other_ref[:, span(c), :WIDTH]).astype(f32), theirs * share)
        numer = (numer + scaled(mix(weights, keys), share)).astype(jnp.bfloat16)
        held[span(c)] = jnp.swapaxes(numer.reshape(heads, step, WIDTH), 0, 1)
        copies.append(pltpu.make_async_copy(held.at[span(c)], out.at[span(c)], sems.at[c]))
        copies[-1].start()
        scores = ahead
    for copy in copies:
        copy.wait()


def prepare_kernel(order_ref, place_ref, latent_ref, rope_ref, out, seen_ref):
    out[:, :, :WIDTH] = jnp.swapaxes(latent_ref[...], 0, 1)
    for h in range(4):
        rope = rope_ref[:, h * 64 : h * 64 + 64]
        out[h, :, WIDTH:] = jnp.concatenate([rope, jnp.zeros_like(rope)], axis=1)

    @pl.when(pl.program_id(0) == 0)
    def _():
        fill_seen(order_ref, place_ref, seen_ref)


def prepare(order, place, latent, rope):
    rows, heads, _ = latent.shape
    return pl.pallas_call(
        prepare_kernel,
        grid=(4,),
        out_shape=[
            jax.ShapeDtypeStruct((heads, rows, QUERY), jnp.bfloat16),
            jax.ShapeDtypeStruct((16, HALF), jnp.int32),
        ],
        in_specs=[
            SM,
            SM,
            pl.BlockSpec((rows // 4, heads, WIDTH), lambda i: (i, 0, 0)),
            pl.BlockSpec((rows // 4, heads * 64), lambda i: (i, 0)),
        ],
        out_specs=[
            pl.BlockSpec((heads, rows // 4, QUERY), lambda i: (0, i, 0)),
            pl.BlockSpec((16, HALF), lambda i: (0, 0)),
        ],
        compiler_params=pltpu.CompilerParams(vmem_limit_bytes=VMEM_MIB * 2**20),
        cost_estimate=pl.CostEstimate(flops=1 << 30, bytes_accessed=2_000_000, transcendentals=0),
        name="prepare",
    )(order, place, latent, rope)


def spread_kernel(cache_ref, out, held, sems):
    first = pl.multiple_of(lax.axis_index("co") * HALF, HALF)
    load = pltpu.make_async_copy(cache_ref.at[:, pl.ds(first, HALF)], held, sems.at[0])
    load.start()
    load.wait()
    stores = [pltpu.make_async_copy(held, out.at[i], sems.at[1 + i]) for i in range(4)]
    for store in stores:
        store.start()
    for store in stores:
        store.wait()


def spread(cache):
    rows = cache.shape[0]
    hbm = pl.BlockSpec(memory_space=pltpu.HBM)
    copies = pl.pallas_call(
        spread_kernel,
        in_specs=[hbm],
        out_specs=hbm,
        out_shape=jax.ShapeDtypeStruct((4, rows, HALF), cache.dtype),
        scratch_shapes=[pltpu.VMEM((rows, HALF), cache.dtype), pltpu.SemaphoreType.DMA((5,))],
        compiler_params=pltpu.CompilerParams(vmem_limit_bytes=VMEM_MIB * 2**20),
        name="spread",
    )(cache)
    return copies.reshape(4 * rows, HALF)


def call(kernel, out_shape, pieces, args, aliases=None, scratch=(), out_spec=VM):
    heads, keys = 4, pieces * HALF
    cost = pl.CostEstimate(
        flops=2 * heads * 256 * keys * (WIDTH * 2 + 64) * 2,
        bytes_accessed=4_000_000,
        transcendentals=heads * 256 * keys,
    )
    return pl.pallas_call(
        kernel,
        out_shape=out_shape,
        in_specs=[VM] * len(args),
        out_specs=[VM] * len(out_shape) if isinstance(out_shape, list) else out_spec,
        input_output_aliases=aliases or {},
        scratch_shapes=scratch,
        compiler_params=pltpu.CompilerParams(vmem_limit_bytes=VMEM_MIB * 2**20),
        cost_estimate=cost,
    )(*args)


def attend(query_latent, query_rope, latent_cache, group_order):
    rows, heads, _ = query_latent.shape
    core = lax.axis_index("co")
    x, y = lax.axis_index("x"), lax.axis_index("yl")
    where = [group_order, jnp.stack([core, x, y]).astype(jnp.int32)]
    copies = spread(in_hbm(latent_cache))
    bundle = lax.all_to_all(copies, RING, 0, 0, axis_index_groups=near_groups(), tiled=True)
    queries, seen = prepare(*where, in_hbm(query_latent), in_hbm(query_rope))
    bundle = bundle.reshape(4, WIDTH + 64, HALF)
    far = []
    for shift in (1, -1, 2):
        far.append(split_permute(bundle, shift, 1))
    twin = lax.ppermute(queries, "co", [(0, 1), (1, 0)])

    state = jax.ShapeDtypeStruct((heads, rows, STATE), f32)

    def more(queries, states, *parts):
        count = len(queries)
        kernel = functools.partial(more_kernel, parts, count)
        args = [seen, *queries, *states, *(far[part] for part in parts)]
        aliases = {1 + count + i: i for i in range(count)}
        return call(kernel, [state] * count, 4 * len(parts) * count, args, aliases)

    packed = jax.ShapeDtypeStruct(twin.shape, twin.dtype)
    args = [seen, queries, twin, bundle]
    own, sib, twin = call(near_kernel, [state, state, packed], 8, args)
    own, sib = more([queries, twin], [own, sib], 2)
    (sib,) = more([twin], [sib], 0)
    send = functools.partial(send_kernel, (1,))
    sib = call(send, packed, 4, [seen, twin, sib, far[1]])
    other = lax.ppermute(sib, "co", [(0, 1), (1, 0)])
    (own,) = more([queries], [own], 0)
    out = jax.ShapeDtypeStruct((rows, heads, WIDTH), jnp.bfloat16)
    last = functools.partial(last_kernel, (1,))
    scratch = [pltpu.VMEM((rows, heads, WIDTH), jnp.bfloat16), pltpu.SemaphoreType.DMA((4,))]
    args = [seen, queries, own, other, far[1]]
    hbm = pl.BlockSpec(memory_space=pltpu.HBM)
    return call(last, out, 4, args, scratch=scratch, out_spec=hbm)


def solution(mesh):
    depth = mesh.shape["expert"] // 4
    torus = Mesh(mesh.devices.reshape(depth, 2, 2, 4, 4), ("z",) + RING)
    expert, ctx = ("z", "yh", "co"), ("x", "yl")
    placed = (P(ctx, expert, None), P(ctx, expert), P(None, ctx), P())
    return jax.shard_map(
        attend, mesh=torus, in_specs=placed, out_specs=P(ctx, expert, None), check_vma=False
    )
```

```python
import functools
import math

import jax
import jax.numpy as jnp
from jax import lax
from jax.experimental import pallas as pl
from jax.experimental.pallas import tpu as pltpu
from jax.sharding import Mesh
from jax.sharding import PartitionSpec as P


LOG_SCALE = 192.0 ** (-0.5) * math.log2(math.e)
MASKED = -1e30
FLOOR = -1e29
RING = ("yh", "co", "x", "yl")
HALF = 128
VMEM_MIB = 16
QUERY = 640
USED = 576
OUTER = (-1, 1, 2)
WIDTH = 512
STATE = 768
PEAK = slice(512, 640)
TOTAL = slice(640, 768)
f32 = jnp.float32
VM = pl.BlockSpec(memory_space=pltpu.VMEM)
SM = pl.BlockSpec(memory_space=pltpu.SMEM)


def split_permute(value, shift, along):
    pairs = []
    for y in range(8):
        for core in range(2):
            for x in range(4):
                to_y, to_x = y, x
                if (core == 0) == (along == 0):
                    step = shift
                    if shift == 2 and y % 2:
                        step = -2
                    to_y = (y + step) % 8
                else:
                    to_x = (x + shift) % 4
                at = lambda u, v: (((u // 4) * 2 + core) * 4 + v) * 4 + u % 4
                pairs.append((at(y, x), at(to_y, to_x)))
    return lax.ppermute(value, RING, pairs)


def in_hbm(value):
    return pltpu.with_memory_space_constraint(value, pltpu.HBM)


def near_groups():
    groups = []
    for half in range(2):
        at = lambda core, x, y: ((half * 2 + core) * 4 + x) * 4 + y
        groups += [[at(0, x, y) for y in range(4)] for x in range(4)]
        groups += [[at(1, x, y) for x in range(4)] for y in range(4)]
    return groups


def keys_of(refs):
    tiles = [ref[i] for ref in refs for i in range(ref.shape[0])]
    return jnp.concatenate(tiles, axis=1)


def scores_of(queries, keys):
    return jnp.dot(queries[:, :USED], keys, preferred_element_type=f32)


def mix(weights, keys):
    return lax.dot_general(
        weights, keys[:WIDTH], (((1,), (1,)), ((), ())), preferred_element_type=f32
    )


def soften(parts, peak, total):
    top = parts[0]
    for part in parts[1:]:
        top = jnp.maximum(top, part)
    row_top = jnp.max(top, axis=1, keepdims=True)
    new_peak = jnp.maximum(peak, jnp.broadcast_to(row_top, top.shape))
    offset = new_peak * LOG_SCALE
    weights = [jnp.exp2(part * LOG_SCALE - offset) for part in parts]
    keep = jnp.exp2(peak * LOG_SCALE - offset)
    added = weights[0]
    for part in weights[1:]:
        added = added + part
    total = added if total is None else total * keep + added
    return jnp.concatenate([w.astype(jnp.bfloat16) for w in weights], axis=1), new_peak, total, keep


def pieces_of(scores):
    return [scores[:, i : i + HALF] for i in range(0, scores.shape[1], HALF)]


def block_of(place, inner, outer):
    core, x, y = place
    at_y = jnp.where(core == 0, inner, (y + outer + 4) % 4)
    at_x = jnp.where(core == 0, (x + outer + 4) % 4, inner)
    return at_x * 4 + at_y


def fill_seen(order_ref, place_ref, seen_ref):
    place = place_ref[0], place_ref[1], place_ref[2]
    mine = order_ref[place[1] * 4 + place[2]]
    for i in range(16):
        order = order_ref[block_of(place, i % 4, (0, *OUTER)[i // 4])]
        limit = jnp.where(order < mine, 4096, -4096)
        limit = jnp.where(order == mine, -HALF * place[0], limit)
        seen_ref[i : i + 1, :] = jnp.full((1, HALF), limit, jnp.int32)


def masked_pieces(scores, seen_ref, parts):
    pieces = pieces_of(scores)
    for i, part in enumerate(pieces):
        row = 4 + 4 * parts[i // 4] + i % 4
        pieces[i] = jnp.where(seen_ref[row : row + 1, :] > 0, part, MASKED)
    return pieces


def scaled(numer, factor):
    return jnp.concatenate([part * factor for part in pieces_of(numer)], axis=1)


def put_state(ref, h, numer, peak, total):
    ref[h, :, :WIDTH] = numer
    ref[h, :, PEAK] = peak
    ref[h, :, TOTAL] = total


def near_kernel(seen_ref, own_ref, twin_ref, kv_ref, far_ref, own_out, sib_out, keep_ref):
    keys = keys_of([kv_ref, far_ref])
    rows = own_ref.shape[1]
    lane = lax.broadcasted_iota(jnp.int32, (rows, HALF), 1)
    ahead_by = lane - lax.broadcasted_iota(jnp.int32, (rows, HALF), 0)
    work = [(own_ref, own_out, h) for h in range(4)] + [(twin_ref, sib_out, h) for h in range(4)]
    scores = scores_of(own_ref[0], keys)
    for i, (_, out, h) in enumerate(work):
        ahead = None
        if i + 1 < len(work):
            ahead = scores_of(work[i + 1][0][work[i + 1][2]], keys)
        parts = [
            jnp.where(ahead_by <= seen_ref[j : j + 1, :], part, MASKED)
            for j, part in enumerate(pieces_of(scores[:, : 4 * HALF]))
        ]
        parts += masked_pieces(scores[:, 4 * HALF :], seen_ref, (2,))
        floor = jnp.full((rows, HALF), FLOOR, f32)
        weights, peak, total, _ = soften(parts, floor, None)
        put_state(out, h, mix(weights, keys), peak, total)
        scores = ahead
    keep_ref[...] = twin_ref[...]


def more_kernel(parts_in, count, seen_ref, *refs):
    queries, states = refs[:count], refs[count : 2 * count]
    outs = refs[len(refs) - count :]
    keys = keys_of(refs[2 * count : len(refs) - count])
    work = [(q, s, out, h) for q, s, out in zip(queries, states, outs) for h in range(4)]
    scores = scores_of(work[0][0][0], keys)
    for i, (_, state, out, h) in enumerate(work):
        ahead = None
        if i + 1 < len(work):
            ahead = scores_of(work[i + 1][0][work[i + 1][3]], keys)
        parts = masked_pieces(scores, seen_ref, parts_in)
        weights, peak, total, keep = soften(parts, state[h, :, PEAK], state[h, :, TOTAL])
        numer = scaled(state[h, :, :WIDTH], keep) + mix(weights, keys)
        put_state(out, h, numer, peak, total)
        scores = ahead


def send_kernel(parts_in, seen_ref, q_ref, state_ref, *refs):
    keys = keys_of(refs[:-1])
    out = refs[-1]
    scores = scores_of(q_ref[0], keys)
    rows = q_ref.shape[1]
    lane = lax.broadcasted_iota(jnp.int32, (rows, HALF), 1)
    for h in range(4):
        ahead = scores_of(q_ref[h + 1], keys) if h < 3 else None
        parts = masked_pieces(scores, seen_ref, parts_in)
        weights, peak, total, keep = soften(parts, state_ref[h, :, PEAK], state_ref[h, :, TOTAL])
        total = jnp.broadcast_to(jnp.sum(total, axis=1, keepdims=True), (rows, HALF))
        some = total > 0.0
        share = jnp.where(some, 1.0 / jnp.where(some, total, 1.0), 0.0)
        size = jnp.log2(jnp.where(some, total, 1.0)) + peak * LOG_SCALE
        size = jnp.where(some, size, FLOOR)
        high = size.astype(jnp.bfloat16).astype(f32)
        middle = (size - high).astype(jnp.bfloat16).astype(f32)
        low = size - high - middle
        tag = jnp.where(lane == 0, high, jnp.where(lane == 1, middle, low))
        out[h, :, WIDTH:] = jnp.where(lane < 3, tag, 0.0).astype(jnp.bfloat16)
        numer = scaled(state_ref[h, :, :WIDTH], keep * share)
        for i, part in enumerate(pieces_of(mix(weights, keys))):
            span = slice(i * HALF, (i + 1) * HALF)
            out[h, :, span] = (numer[:, span] + part * share).astype(jnp.bfloat16)
        scores = ahead


def last_kernel(parts_in, seen_ref, q_ref, state_ref, other_ref, kv_ref, out, held, sems):
    keys = keys_of([kv_ref])
    heads, rows, _ = q_ref.shape
    step = rows // 4
    span = lambda c: slice(c * step, (c + 1) * step)
    flat = lambda value: value.reshape(heads * step, value.shape[-1])
    scores = scores_of(flat(q_ref[:, span(0), :]), keys)
    copies = []
    for c in range(4):
        ahead = scores_of(flat(q_ref[:, span(c + 1), :]), keys) if c < 3 else None
        parts = masked_pieces(scores, seen_ref, parts_in)
        peak = flat(state_ref[:, span(c), PEAK])
        size = flat(other_ref[:, span(c), WIDTH:]).astype(f32)
        size = jnp.broadcast_to(jnp.sum(size, axis=1, keepdims=True), peak.shape)
        floor = jnp.maximum(peak, size * (1.0 / LOG_SCALE))
        weights, top, added, _ = soften(parts, floor, None)
        mine = jnp.exp2((peak - top) * LOG_SCALE)
        theirs = jnp.exp2(size - top * LOG_SCALE)
        total = flat(state_ref[:, span(c), TOTAL]) * mine + added
        total = jnp.sum(total, axis=1, keepdims=True)
        share = 1.0 / (jnp.broadcast_to(total, peak.shape) + theirs)
        numer = scaled(flat(state_ref[:, span(c), :WIDTH]), mine * share)
        numer = numer + scaled(flat(other_ref[:, span(c), :WIDTH]).astype(f32), theirs * share)
        numer = (numer + scaled(mix(weights, keys), share)).astype(jnp.bfloat16)
        held[span(c)] = jnp.swapaxes(numer.reshape(heads, step, WIDTH), 0, 1)
        copies.append(pltpu.make_async_copy(held.at[span(c)], out.at[span(c)], sems.at[c]))
        copies[-1].start()
        scores = ahead
    for copy in copies:
        copy.wait()


def prepare_kernel(order_ref, place_ref, latent_ref, rope_ref, out, seen_ref):
    out[:, :, :WIDTH] = jnp.swapaxes(latent_ref[...], 0, 1)
    for h in range(4):
        rope = rope_ref[:, h * 64 : h * 64 + 64]
        out[h, :, WIDTH:] = jnp.concatenate([rope, jnp.zeros_like(rope)], axis=1)

    @pl.when(pl.program_id(0) == 0)
    def _():
        fill_seen(order_ref, place_ref, seen_ref)


def prepare(order, place, latent, rope):
    rows, heads, _ = latent.shape
    return pl.pallas_call(
        prepare_kernel,
        grid=(4,),
        out_shape=[
            jax.ShapeDtypeStruct((heads, rows, QUERY), jnp.bfloat16),
            jax.ShapeDtypeStruct((16, HALF), jnp.int32),
        ],
        in_specs=[
            SM,
            SM,
            pl.BlockSpec((rows // 4, heads, WIDTH), lambda i: (i, 0, 0)),
            pl.BlockSpec((rows // 4, heads * 64), lambda i: (i, 0)),
        ],
        out_specs=[
            pl.BlockSpec((heads, rows // 4, QUERY), lambda i: (0, i, 0)),
            pl.BlockSpec((16, HALF), lambda i: (0, 0)),
        ],
        compiler_params=pltpu.CompilerParams(vmem_limit_bytes=VMEM_MIB * 2**20),
        cost_estimate=pl.CostEstimate(flops=1 << 30, bytes_accessed=2_000_000, transcendentals=0),
        name="prepare",
    )(order, place, latent, rope)


def spread_kernel(cache_ref, out, held, sems):
    first = pl.multiple_of(lax.axis_index("co") * HALF, HALF)
    load = pltpu.make_async_copy(cache_ref.at[:, pl.ds(first, HALF)], held, sems.at[0])
    load.start()
    load.wait()
    stores = [pltpu.make_async_copy(held, out.at[i], sems.at[1 + i]) for i in range(4)]
    for store in stores:
        store.start()
    for store in stores:
        store.wait()


def spread(cache):
    rows = cache.shape[0]
    hbm = pl.BlockSpec(memory_space=pltpu.HBM)
    copies = pl.pallas_call(
        spread_kernel,
        in_specs=[hbm],
        out_specs=hbm,
        out_shape=jax.ShapeDtypeStruct((4, rows, HALF), cache.dtype),
        scratch_shapes=[pltpu.VMEM((rows, HALF), cache.dtype), pltpu.SemaphoreType.DMA((5,))],
        compiler_params=pltpu.CompilerParams(vmem_limit_bytes=VMEM_MIB * 2**20),
        name="spread",
    )(cache)
    return copies.reshape(4 * rows, HALF)


def call(kernel, out_shape, pieces, args, aliases=None, scratch=(), out_spec=VM):
    heads, keys = 4, pieces * HALF
    cost = pl.CostEstimate(
        flops=2 * heads * 256 * keys * (WIDTH * 2 + 64) * 2,
        bytes_accessed=4_000_000,
        transcendentals=heads * 256 * keys,
    )
    return pl.pallas_call(
        kernel,
        out_shape=out_shape,
        in_specs=[VM] * len(args),
        out_specs=[VM] * len(out_shape) if isinstance(out_shape, list) else out_spec,
        input_output_aliases=aliases or {},
        scratch_shapes=scratch,
        compiler_params=pltpu.CompilerParams(vmem_limit_bytes=VMEM_MIB * 2**20),
        cost_estimate=cost,
    )(*args)


def attend(query_latent, query_rope, latent_cache, group_order):
    rows, heads, _ = query_latent.shape
    core = lax.axis_index("co")
    x, y = lax.axis_index("x"), lax.axis_index("yl")
    where = [group_order, jnp.stack([core, x, y]).astype(jnp.int32)]
    copies = spread(in_hbm(latent_cache))
    bundle = lax.all_to_all(copies, RING, 0, 0, axis_index_groups=near_groups(), tiled=True)
    queries, seen = prepare(*where, in_hbm(query_latent), in_hbm(query_rope))
    bundle = bundle.reshape(4, WIDTH + 64, HALF)
    far = []
    for shift in (1, -1, 2):
        far.append(split_permute(bundle, shift, 1))
    twin = lax.ppermute(queries, "co", [(0, 1), (1, 0)])

    state = jax.ShapeDtypeStruct((heads, rows, STATE), f32)

    def more(queries, states, *parts):
        count = len(queries)
        kernel = functools.partial(more_kernel, parts, count)
        args = [seen, *queries, *states, *(far[part] for part in parts)]
        aliases = {1 + count + i: i for i in range(count)}
        return call(kernel, [state] * count, 4 * len(parts) * count, args, aliases)

    packed = jax.ShapeDtypeStruct(twin.shape, twin.dtype)
    args = [seen, queries, twin, bundle, far[2]]
    own, sib, twin = call(near_kernel, [state, state, packed], 16, args)
    (sib,) = more([twin], [sib], 0)
    send = functools.partial(send_kernel, (1,))
    sib = call(send, packed, 4, [seen, twin, sib, far[1]])
    other = lax.ppermute(sib, "co", [(0, 1), (1, 0)])
    (own,) = more([queries], [own], 0)
    out = jax.ShapeDtypeStruct((rows, heads, WIDTH), jnp.bfloat16)
    last = functools.partial(last_kernel, (1,))
    scratch = [pltpu.VMEM((rows, heads, WIDTH), jnp.bfloat16), pltpu.SemaphoreType.DMA((4,))]
    args = [seen, queries, own, other, far[1]]
    hbm = pl.BlockSpec(memory_space=pltpu.HBM)
    return call(last, out, 4, args, scratch=scratch, out_spec=hbm)


def solution(mesh):
    depth = mesh.shape["expert"] // 4
    torus = Mesh(mesh.devices.reshape(depth, 2, 2, 4, 4), ("z",) + RING)
    expert, ctx = ("z", "yh", "co"), ("x", "yl")
    placed = (P(ctx, expert, None), P(ctx, expert), P(None, ctx), P())
    return jax.shard_map(
        attend, mesh=torus, in_specs=placed, out_specs=P(ctx, expert, None), check_vma=False
    )
```

```python
import functools
import math

import jax
import jax.numpy as jnp
from jax import lax
from jax.experimental import pallas as pl
from jax.experimental.pallas import tpu as pltpu
from jax.sharding import Mesh
from jax.sharding import PartitionSpec as P


LOG_SCALE = 192.0 ** (-0.5) * math.log2(math.e)
MASKED = -1e30
FLOOR = -1e29
RING = ("yh", "co", "x", "yl")
HALF = 128
VMEM_MIB = 16
QUERY = 640
USED = 576
OUTER = (-1, 1, 2)
WIDTH = 512
STATE = 768
PEAK = slice(512, 640)
TOTAL = slice(640, 768)
f32 = jnp.float32
VM = pl.BlockSpec(memory_space=pltpu.VMEM)
SM = pl.BlockSpec(memory_space=pltpu.SMEM)


def split_permute(value, shift, along):
    pairs = []
    for y in range(8):
        for core in range(2):
            for x in range(4):
                to_y, to_x = y, x
                if (core == 0) == (along == 0):
                    step = shift
                    if shift == 2 and y % 2:
                        step = -2
                    to_y = (y + step) % 8
                else:
                    to_x = (x + shift) % 4
                at = lambda u, v: (((u // 4) * 2 + core) * 4 + v) * 4 + u % 4
                pairs.append((at(y, x), at(to_y, to_x)))
    return lax.ppermute(value, RING, pairs)


def in_hbm(value):
    return pltpu.with_memory_space_constraint(value, pltpu.HBM)


def near_groups():
    groups = []
    for half in range(2):
        at = lambda core, x, y: ((half * 2 + core) * 4 + x) * 4 + y
        groups += [[at(0, x, y) for y in range(4)] for x in range(4)]
        groups += [[at(1, x, y) for x in range(4)] for y in range(4)]
    return groups


def keys_of(refs):
    tiles = [ref[i] for ref in refs for i in range(ref.shape[0])]
    return jnp.concatenate(tiles, axis=1)


def scores_of(queries, keys):
    return jnp.dot(queries[:, :USED], keys, preferred_element_type=f32)


def mix(weights, keys):
    return lax.dot_general(
        weights, keys[:WIDTH], (((1,), (1,)), ((), ())), preferred_element_type=f32
    )


def soften(parts, peak, total):
    top = parts[0]
    for part in parts[1:]:
        top = jnp.maximum(top, part)
    row_top = jnp.max(top, axis=1, keepdims=True)
    new_peak = jnp.maximum(peak, jnp.broadcast_to(row_top, top.shape))
    offset = new_peak * LOG_SCALE
    weights = [jnp.exp2(part * LOG_SCALE - offset) for part in parts]
    keep = jnp.exp2(peak * LOG_SCALE - offset)
    added = weights[0]
    for part in weights[1:]:
        added = added + part
    total = added if total is None else total * keep + added
    return jnp.concatenate([w.astype(jnp.bfloat16) for w in weights], axis=1), new_peak, total, keep


def pieces_of(scores):
    return [scores[:, i : i + HALF] for i in range(0, scores.shape[1], HALF)]


def block_of(place, inner, outer):
    core, x, y = place
    at_y = jnp.where(core == 0, inner, (y + outer + 4) % 4)
    at_x = jnp.where(core == 0, (x + outer + 4) % 4, inner)
    return at_x * 4 + at_y


def fill_seen(order_ref, place_ref, seen_ref):
    place = place_ref[0], place_ref[1], place_ref[2]
    mine = order_ref[place[1] * 4 + place[2]]
    for i in range(16):
        order = order_ref[block_of(place, i % 4, (0, *OUTER)[i // 4])]
        limit = jnp.where(order < mine, 4096, -4096)
        limit = jnp.where(order == mine, -HALF * place[0], limit)
        seen_ref[i : i + 1, :] = jnp.full((1, HALF), limit, jnp.int32)


def masked_pieces(scores, seen_ref, parts):
    pieces = pieces_of(scores)
    for i, part in enumerate(pieces):
        row = 4 + 4 * parts[i // 4] + i % 4
        pieces[i] = jnp.where(seen_ref[row : row + 1, :] > 0, part, MASKED)
    return pieces


def scaled(numer, factor):
    return jnp.concatenate([part * factor for part in pieces_of(numer)], axis=1)


def put_state(ref, h, numer, peak, total):
    ref[h, :, :WIDTH] = numer
    ref[h, :, PEAK] = peak
    ref[h, :, TOTAL] = total


def near_kernel(seen_ref, own_ref, twin_ref, kv_ref, far_ref, own_out, sib_out, keep_ref):
    keys = keys_of([kv_ref, far_ref])
    rows = own_ref.shape[1]
    lane = lax.broadcasted_iota(jnp.int32, (rows, HALF), 1)
    ahead_by = lane - lax.broadcasted_iota(jnp.int32, (rows, HALF), 0)
    work = [(own_ref, own_out, h) for h in range(4)] + [(twin_ref, sib_out, h) for h in range(4)]
    scores = scores_of(own_ref[0], keys)
    for i, (_, out, h) in enumerate(work):
        ahead = None
        if i + 1 < len(work):
            ahead = scores_of(work[i + 1][0][work[i + 1][2]], keys)
        parts = [
            jnp.where(ahead_by <= seen_ref[j : j + 1, :], part, MASKED)
            for j, part in enumerate(pieces_of(scores[:, : 4 * HALF]))
        ]
        parts += masked_pieces(scores[:, 4 * HALF :], seen_ref, (2,))
        floor = jnp.full((rows, HALF), FLOOR, f32)
        weights, peak, total, _ = soften(parts, floor, None)
        put_state(out, h, mix(weights, keys), peak, total)
        scores = ahead
    keep_ref[...] = twin_ref[...]


def more_kernel(parts_in, count, seen_ref, *refs):
    queries, states = refs[:count], refs[count : 2 * count]
    outs = refs[len(refs) - count :]
    keys = keys_of(refs[2 * count : len(refs) - count])
    work = [(q, s, out, h) for q, s, out in zip(queries, states, outs) for h in range(4)]
    scores = scores_of(work[0][0][0], keys)
    for i, (_, state, out, h) in enumerate(work):
        ahead = None
        if i + 1 < len(work):
            ahead = scores_of(work[i + 1][0][work[i + 1][3]], keys)
        parts = masked_pieces(scores, seen_ref, parts_in)
        weights, peak, total, keep = soften(parts, state[h, :, PEAK], state[h, :, TOTAL])
        numer = scaled(state[h, :, :WIDTH], keep) + mix(weights, keys)
        put_state(out, h, numer, peak, total)
        scores = ahead


def send_kernel(parts_in, seen_ref, q_ref, state_ref, *refs):
    keys = keys_of(refs[:-1])
    out = refs[-1]
    scores = scores_of(q_ref[0], keys)
    rows = q_ref.shape[1]
    lane = lax.broadcasted_iota(jnp.int32, (rows, HALF), 1)
    for h in range(4):
        ahead = scores_of(q_ref[h + 1], keys) if h < 3 else None
        parts = masked_pieces(scores, seen_ref, parts_in)
        weights, peak, total, keep = soften(parts, state_ref[h, :, PEAK], state_ref[h, :, TOTAL])
        total = jnp.broadcast_to(jnp.sum(total, axis=1, keepdims=True), (rows, HALF))
        some = total > 0.0
        share = jnp.where(some, 1.0 / jnp.where(some, total, 1.0), 0.0)
        size = jnp.log2(jnp.where(some, total, 1.0)) + peak * LOG_SCALE
        size = jnp.where(some, size, FLOOR)
        high = size.astype(jnp.bfloat16).astype(f32)
        middle = (size - high).astype(jnp.bfloat16).astype(f32)
        low = size - high - middle
        tag = jnp.where(lane == 0, high, jnp.where(lane == 1, middle, low))
        out[h, :, WIDTH:] = jnp.where(lane < 3, tag, 0.0).astype(jnp.bfloat16)
        numer = scaled(state_ref[h, :, :WIDTH], keep * share)
        for i, part in enumerate(pieces_of(mix(weights, keys))):
            span = slice(i * HALF, (i + 1) * HALF)
            out[h, :, span] = (numer[:, span] + part * share).astype(jnp.bfloat16)
        scores = ahead


def last_kernel(parts_in, seen_ref, q_ref, state_ref, other_ref, kv_ref, out, held, sems):
    keys = keys_of([kv_ref])
    heads, rows, _ = q_ref.shape
    step = rows // 4
    span = lambda c: slice(c * step, (c + 1) * step)
    flat = lambda value: value.reshape(heads * step, value.shape[-1])
    scores = scores_of(flat(q_ref[:, span(0), :]), keys)
    copies = []
    for c in range(4):
        ahead = scores_of(flat(q_ref[:, span(c + 1), :]), keys) if c < 3 else None
        parts = masked_pieces(scores, seen_ref, parts_in)
        peak = flat(state_ref[:, span(c), PEAK])
        size = flat(other_ref[:, span(c), WIDTH:]).astype(f32)
        size = jnp.broadcast_to(jnp.sum(size, axis=1, keepdims=True), peak.shape)
        floor = jnp.maximum(peak, size * (1.0 / LOG_SCALE))
        weights, top, added, _ = soften(parts, floor, None)
        mine = jnp.exp2((peak - top) * LOG_SCALE)
        theirs = jnp.exp2(size - top * LOG_SCALE)
        total = flat(state_ref[:, span(c), TOTAL]) * mine + added
        total = jnp.sum(total, axis=1, keepdims=True)
        share = 1.0 / (jnp.broadcast_to(total, peak.shape) + theirs)
        numer = scaled(flat(state_ref[:, span(c), :WIDTH]), mine * share)
        numer = numer + scaled(flat(other_ref[:, span(c), :WIDTH]).astype(f32), theirs * share)
        numer = (numer + scaled(mix(weights, keys), share)).astype(jnp.bfloat16)
        held[span(c)] = jnp.swapaxes(numer.reshape(heads, step, WIDTH), 0, 1)
        copies.append(pltpu.make_async_copy(held.at[span(c)], out.at[span(c)], sems.at[c]))
        copies[-1].start()
        scores = ahead
    for copy in copies:
        copy.wait()


def prepare_kernel(order_ref, place_ref, latent_ref, rope_ref, out, seen_ref):
    out[:, :, :WIDTH] = jnp.swapaxes(latent_ref[...], 0, 1)
    for h in range(4):
        rope = rope_ref[:, h * 64 : h * 64 + 64]
        out[h, :, WIDTH:] = jnp.concatenate([rope, jnp.zeros_like(rope)], axis=1)

    @pl.when(pl.program_id(0) == 0)
    def _():
        fill_seen(order_ref, place_ref, seen_ref)


def prepare(order, place, latent, rope):
    rows, heads, _ = latent.shape
    return pl.pallas_call(
        prepare_kernel,
        grid=(4,),
        out_shape=[
            jax.ShapeDtypeStruct((heads, rows, QUERY), jnp.bfloat16),
            jax.ShapeDtypeStruct((16, HALF), jnp.int32),
        ],
        in_specs=[
            SM,
            SM,
            pl.BlockSpec((rows // 4, heads, WIDTH), lambda i: (i, 0, 0)),
            pl.BlockSpec((rows // 4, heads * 64), lambda i: (i, 0)),
        ],
        out_specs=[
            pl.BlockSpec((heads, rows // 4, QUERY), lambda i: (0, i, 0)),
            pl.BlockSpec((16, HALF), lambda i: (0, 0)),
        ],
        compiler_params=pltpu.CompilerParams(vmem_limit_bytes=VMEM_MIB * 2**20),
        cost_estimate=pl.CostEstimate(flops=1 << 30, bytes_accessed=2_000_000, transcendentals=0),
        name="prepare",
    )(order, place, latent, rope)


def spread_kernel(cache_ref, out, held, sems):
    first = pl.multiple_of(lax.axis_index("co") * HALF, HALF)
    load = pltpu.make_async_copy(cache_ref.at[:, pl.ds(first, HALF)], held, sems.at[0])
    load.start()
    load.wait()
    stores = [pltpu.make_async_copy(held, out.at[i], sems.at[1 + i]) for i in range(4)]
    for store in stores:
        store.start()
    for store in stores:
        store.wait()


def spread(cache):
    rows = cache.shape[0]
    hbm = pl.BlockSpec(memory_space=pltpu.HBM)
    copies = pl.pallas_call(
        spread_kernel,
        in_specs=[hbm],
        out_specs=hbm,
        out_shape=jax.ShapeDtypeStruct((4, rows, HALF), cache.dtype),
        scratch_shapes=[pltpu.VMEM((rows, HALF), cache.dtype), pltpu.SemaphoreType.DMA((5,))],
        compiler_params=pltpu.CompilerParams(vmem_limit_bytes=VMEM_MIB * 2**20),
        name="spread",
    )(cache)
    return copies.reshape(4 * rows, HALF)


def call(kernel, out_shape, pieces, args, aliases=None, scratch=(), out_spec=VM):
    heads, keys = 4, pieces * HALF
    cost = pl.CostEstimate(
        flops=2 * heads * 256 * keys * (WIDTH * 2 + 64) * 2,
        bytes_accessed=4_000_000,
        transcendentals=heads * 256 * keys,
    )
    return pl.pallas_call(
        kernel,
        out_shape=out_shape,
        in_specs=[VM] * len(args),
        out_specs=[VM] * len(out_shape) if isinstance(out_shape, list) else out_spec,
        input_output_aliases=aliases or {},
        scratch_shapes=scratch,
        compiler_params=pltpu.CompilerParams(vmem_limit_bytes=VMEM_MIB * 2**20),
        cost_estimate=cost,
    )(*args)


def attend(query_latent, query_rope, latent_cache, group_order):
    rows, heads, _ = query_latent.shape
    core = lax.axis_index("co")
    x, y = lax.axis_index("x"), lax.axis_index("yl")
    where = [group_order, jnp.stack([core, x, y]).astype(jnp.int32)]
    copies = spread(in_hbm(latent_cache))
    bundle = lax.all_to_all(copies, RING, 0, 0, axis_index_groups=near_groups(), tiled=True)
    queries, seen = prepare(*where, in_hbm(query_latent), in_hbm(query_rope))
    bundle = bundle.reshape(4, WIDTH + 64, HALF)
    far = []
    for shift in (1, -1, 2):
        far.append(split_permute(bundle, shift, 1))
    twin = lax.ppermute(queries, "co", [(0, 1), (1, 0)])

    state = jax.ShapeDtypeStruct((heads, rows, STATE), f32)

    def more(queries, states, *parts):
        count = len(queries)
        kernel = functools.partial(more_kernel, parts, count)
        args = [seen, *queries, *states, *(far[part] for part in parts)]
        aliases = {1 + count + i: i for i in range(count)}
        return call(kernel, [state] * count, 4 * len(parts) * count, args, aliases)

    packed = jax.ShapeDtypeStruct(twin.shape, twin.dtype)
    args = [seen, queries, twin, bundle, far[2]]
    own, sib, twin = call(near_kernel, [state, state, packed], 16, args)
    send = functools.partial(send_kernel, (0, 1))
    sib = call(send, packed, 8, [seen, twin, sib, far[0], far[1]])
    other = lax.ppermute(sib, "co", [(0, 1), (1, 0)])
    (own,) = more([queries], [own], 0)
    out = jax.ShapeDtypeStruct((rows, heads, WIDTH), jnp.bfloat16)
    last = functools.partial(last_kernel, (1,))
    scratch = [pltpu.VMEM((rows, heads, WIDTH), jnp.bfloat16), pltpu.SemaphoreType.DMA((4,))]
    args = [seen, queries, own, other, far[1]]
    hbm = pl.BlockSpec(memory_space=pltpu.HBM)
    return call(last, out, 4, args, scratch=scratch, out_spec=hbm)


def solution(mesh):
    depth = mesh.shape["expert"] // 4
    torus = Mesh(mesh.devices.reshape(depth, 2, 2, 4, 4), ("z",) + RING)
    expert, ctx = ("z", "yh", "co"), ("x", "yl")
    placed = (P(ctx, expert, None), P(ctx, expert), P(None, ctx), P())
    return jax.shard_map(
        attend, mesh=torus, in_specs=placed, out_specs=P(ctx, expert, None), check_vma=False
    )
```
